128 devices in a mesh: rep: 1, dp: 64 (over z, y, x), sp: 2 (over core).
Axes of the slice: x: 4, y: 4, z: 4, core: 2. Of those that a mesh axis runs over, the one named last changes fastest.
Arguments:
- hidden: bfloat16 [256, 6144], P(('rep', 'dp'))
- w_query: bfloat16 [6144, 6144], replicated
- w_key: bfloat16 [6144, 1024], replicated
- w_value: bfloat16 [6144, 1024], replicated
- w_out: bfloat16 [6144, 6144], P('sp')
- k_cache: bfloat16 [256, 512, 8, 128], P(('rep', 'dp'), 'sp')
- v_cache: bfloat16 [256, 512, 8, 128], P(('rep', 'dp'), 'sp')
- write_pos: int32 [256], P(('rep', 'dp'))
- valid_len: int32 [256], P(('rep', 'dp'))
Outputs:
- output 1: bfloat16 [256, 6144], P(('rep', 'dp'))
- output 2: bfloat16 [256, 512, 8, 128], P(('rep', 'dp'), 'sp')
- output 3: bfloat16 [256, 512, 8, 128], P(('rep', 'dp'), 'sp')
All inputs are finite; a program needn't handle non-finite values.
Results may differ from the reference program's by a relative error of at most 0.00648903.
Values are sent between devices in bfloat16 or wider.
A program may use at most 1 GiB of HBM per device.

```python
import jax
import jax.numpy as jnp
from jax import lax

MODEL_DIM = 6144
NUM_HEADS = 48
KV_HEADS = 8
HEAD_DIM = 128
BATCH_SIZE = 256
CACHE_LEN = 512
SEGMENTS = 8


def draw_lengths(rng_key):
    keys = jax.random.split(rng_key, 3)
    shortest = CACHE_LEN // 4
    write_pos = jax.random.randint(keys[0], (BATCH_SIZE,), shortest - 1, CACHE_LEN, jnp.int32)
    long_row = jax.random.randint(keys[1], (), 0, BATCH_SIZE, jnp.int32)
    short_row = (long_row + 1 + jax.random.randint(keys[2], (), 0, BATCH_SIZE - 1, jnp.int32)) % BATCH_SIZE
    row_ids = jnp.arange(BATCH_SIZE, dtype=jnp.int32)
    write_pos = jnp.where(row_ids == long_row, CACHE_LEN - 1, write_pos)
    write_pos = jnp.where(row_ids == short_row, shortest - 1, write_pos)
    return write_pos, write_pos + 1


def setup_inputs(seed: int = 0, part: int = 0) -> dict:
    root = jax.random.key(seed)
    shared = jax.random.split(root, 4)
    own = jax.random.split(jax.random.fold_in(root, part), 8)
    seg_len = CACHE_LEN // SEGMENTS
    proj_width = NUM_HEADS * HEAD_DIM
    kv_width = KV_HEADS * HEAD_DIM
    w_query = (jax.random.normal(shared[0], (MODEL_DIM, proj_width), jnp.float32) * MODEL_DIM ** -0.5).astype(jnp.bfloat16)
    w_key = (jax.random.normal(shared[1], (MODEL_DIM, kv_width), jnp.float32) * MODEL_DIM ** -0.5).astype(jnp.bfloat16)
    w_value = (jax.random.normal(shared[2], (MODEL_DIM, kv_width), jnp.float32) * MODEL_DIM ** -0.5).astype(jnp.bfloat16)
    w_out = (jax.random.normal(shared[3], (proj_width, MODEL_DIM), jnp.float32) * proj_width ** -0.5).astype(jnp.bfloat16)
    hidden = jax.random.normal(own[0], (BATCH_SIZE, MODEL_DIM), jnp.float32).astype(jnp.bfloat16)
    cache_shape = (BATCH_SIZE, SEGMENTS, seg_len, KV_HEADS, HEAD_DIM)
    seg_shape = (BATCH_SIZE, SEGMENTS, 1, KV_HEADS, HEAD_DIM)
    flat_shape = (BATCH_SIZE, CACHE_LEN, KV_HEADS, HEAD_DIM)
    k_cache = (jax.random.normal(own[1], cache_shape, jnp.float32) + jax.random.normal(own[2], seg_shape, jnp.float32)).reshape(flat_shape).astype(jnp.bfloat16)
    v_cache = (jax.random.normal(own[3], cache_shape, jnp.float32) + jax.random.normal(own[4], seg_shape, jnp.float32)).reshape(flat_shape).astype(jnp.bfloat16)
    write_pos, valid_len = draw_lengths(own[5])
    return {'hidden': hidden, 'w_query': w_query, 'w_key': w_key, 'w_value': w_value, 'w_out': w_out, 'k_cache': k_cache, 'v_cache': v_cache, 'write_pos': write_pos, 'valid_len': valid_len}


def reference(hidden, w_query, w_key, w_value, w_out, k_cache, v_cache, write_pos, valid_len):
    group_size = NUM_HEADS // KV_HEADS
    query = jnp.dot(hidden, w_query, preferred_element_type=jnp.float32).astype(jnp.bfloat16)
    query = query.reshape(BATCH_SIZE, KV_HEADS, group_size, HEAD_DIM)
    key_new = jnp.dot(hidden, w_key, preferred_element_type=jnp.float32).astype(jnp.bfloat16)
    value_new = jnp.dot(hidden, w_value, preferred_element_type=jnp.float32).astype(jnp.bfloat16)
    positions = jnp.arange(CACHE_LEN, dtype=jnp.int32)
    at_pos = (positions[None, :] == write_pos[:, None])[:, :, None, None]
    k_next = jnp.where(at_pos, key_new.reshape(BATCH_SIZE, 1, KV_HEADS, HEAD_DIM), k_cache)
    v_next = jnp.where(at_pos, value_new.reshape(BATCH_SIZE, 1, KV_HEADS, HEAD_DIM), v_cache)

    def one_row(row_args):
        q_row, k_row, v_row, length = row_args
        scores = jnp.einsum('kgd,skd->kgs', q_row.astype(jnp.float32), k_row.astype(jnp.float32)) * HEAD_DIM ** -0.5
        scores = jnp.where(positions < length, scores, -jnp.inf)
        row_max = jnp.max(scores, axis=-1, keepdims=True)
        weights = jnp.exp(scores - row_max)
        total = jnp.sum(weights, axis=-1, keepdims=True)
        return jnp.einsum('kgs,skd->kgd', weights, v_row.astype(jnp.float32)) / total

    attention = lax.map(one_row, (query, k_next, v_next, valid_len))
    attention = attention.reshape(BATCH_SIZE, NUM_HEADS * HEAD_DIM).astype(jnp.bfloat16)
    attn_out = jnp.dot(attention, w_out, preferred_element_type=jnp.float32).astype(jnp.bfloat16)
    return (attn_out, k_next, v_next)
```

```python
import functools

import jax
import jax.numpy as jnp
from jax import lax
from jax.experimental import pallas as pl
from jax.experimental.pallas import tpu as pltpu
from jax.sharding import PartitionSpec as P

MESH = pl.DeviceIdType.MESH
BF16, F32 = jnp.bfloat16, jnp.float32

ROWS = 4
CHIPS = 4
D = 128
KV = 8
GROUP = 6
HEADS = KV * GROUP
WIDTH = 6144
HALF = WIDTH // 2
COLS = (GROUP + 2) * D
QCOLS = GROUP * D
SEQ = 256
MY = HEADS // 2
KCH = 1024
NCH = 512
NOUT = WIDTH // NCH
NEG = -1e30
EXP2_SCALE = D ** -0.5 * 1.4426950408889634


def step_kernel(y_stride, hidden, w_query, w_key, w_value, w_out, k_cache, v_cache, write_pos,
                attn_out, k_next, v_next,
                pos_smem, gather, x32, w_in, proj, proj_send, proj_recv, q_rows, kbuf, vbuf, w_o,
                part_send, part_recv, part_own, k_exp, v_exp, o_rows, o_lhs, out_send, out_recv,
                sem_misc, sem_w, sem_kv, sem_wo, send_a, recv_a, send_f, recv_f, send_b, recv_b,
                send_x, recv_x, send_p, recv_p, sem_out):
    core = lax.axis_index('sp')
    other = 1 - core
    dp = lax.axis_index('dp')
    xb = lax.rem(dp, 2)
    yb = lax.rem(dp // y_stride, 2)
    dx, dy = 1 - 2 * xb, 1 - 2 * yb
    chip = [dp, dp + dx, dp + y_stride * dy, dp + dx + y_stride * dy]
    spot0 = xb + 2 * yb
    spot = [spot0, spot0 + dx, spot0 + 2 * dy, spot0 + dx + 2 * dy]
    cores = [core, other]
    mine = spot0 * 2 + core

    def dev(r, d):
        return {'dp': chip[r], 'sp': cores[d]}

    peers = [(3, 0), (3, 1), (1, 0), (1, 1), (2, 0), (2, 1), (0, 1)]

    own = [pltpu.make_async_copy(hidden.at[:, pl.ds(h * HALF, HALF)], gather.at[0, h], sem_misc.at[h])
           for h in range(2)]
    for cp in own:
        cp.start()

    def w_copies(k):
        rows = pl.ds(pl.multiple_of(k * KCH, KCH), KCH)
        col_q = pl.ds(pl.multiple_of(mine * QCOLS, D), QCOLS)
        col_k = pl.ds(pl.multiple_of(mine * D, D), D)
        return [pltpu.make_async_copy(w_query.at[rows, col_q], w_in.at[rows, pl.ds(0, QCOLS)], sem_w.at[k, 0]),
                pltpu.make_async_copy(w_key.at[rows, col_k], w_in.at[rows, pl.ds(QCOLS, D)], sem_w.at[k, 1]),
                pltpu.make_async_copy(w_value.at[rows, col_k], w_in.at[rows, pl.ds(QCOLS + D, D)], sem_w.at[k, 2])]

    per_half = HALF // KCH
    for half in (core, other):
        for i in range(per_half):
            for cp in w_copies(half * per_half + i):
                cp.start()

    barrier = pltpu.get_barrier_semaphore()
    for r, d in peers:
        pl.semaphore_signal(barrier, inc=1, device_id=dev(r, d), device_id_type=MESH)
    for cp in own:
        cp.wait()
    for h in range(2):
        x32[h, 0:ROWS, :] = gather[0, h].astype(F32)
    pl.semaphore_wait(barrier, len(peers))

    def a_copy(r):
        return pltpu.make_async_remote_copy(gather.at[0, core], gather.at[r, core], send_a.at[r], recv_a.at[r],
                                            device_id=dev(r, 0), device_id_type=MESH)

    def f_copy(r):
        return pltpu.make_async_remote_copy(gather.at[r, core], gather.at[r, core], send_f.at[r], recv_f.at[r],
                                            device_id=dev(0, 1), device_id_type=MESH)

    for r in (3, 1, 2):
        a_copy(r).start()

    pos_copy = pltpu.make_async_copy(write_pos, pos_smem, sem_misc.at[2])
    pos_copy.start()
    k_load = pltpu.make_async_copy(k_cache, kbuf, sem_kv.at[0])
    v_load = pltpu.make_async_copy(v_cache, vbuf, sem_kv.at[1])
    k_load.start()
    v_load.start()

    def wo_copy(n):
        return pltpu.make_async_copy(w_out.at[:, pl.ds(pl.multiple_of(n * NCH, NCH), NCH)], w_o.at[n], sem_wo.at[n])

    for n in range(NOUT):
        wo_copy(n).start()

    for r in (1, 2, 3):
        a_copy(r).wait_recv()
        f_copy(r).start()
        x32[core, ROWS * r:ROWS * (r + 1), :] = gather[r, core].astype(F32)

    def project(half):
        def body(i, _):
            k = half * per_half + i
            for cp in w_copies(k):
                cp.wait()
            x = x32[half, :, pl.ds(pl.multiple_of(i * KCH, KCH), KCH)].astype(BF16)
            w = w_in[pl.ds(pl.multiple_of(k * KCH, KCH), KCH), :]
            proj[...] += jnp.dot(x, w, preferred_element_type=F32)
            return 0
        lax.fori_loop(0, per_half, body, 0)

    proj[...] = jnp.zeros_like(proj)
    project(core)
    for r in (1, 2, 3):
        f_copy(r).wait_recv()
        x32[other, ROWS * r:ROWS * (r + 1), :] = gather[r, other].astype(F32)
    project(other)

    for r in range(CHIPS):
        proj_send[r] = proj[ROWS * r:ROWS * (r + 1), :].astype(BF16)

    def b_copy(r, d, slot):
        return pltpu.make_async_remote_copy(proj_send.at[r], proj_recv.at[slot], send_b.at[r, d], recv_b.at[slot],
                                            device_id=dev(r, d), device_id_type=MESH)

    for r, d in peers:
        b_copy(r, d, mine).start()
    proj_recv[mine] = proj_send[0]
    pos_copy.wait()
    for r, d in peers:
        b_copy(r, d, spot[r] * 2 + cores[d]).wait_recv()

    for e in range(KV):
        block = proj_recv[e].astype(F32)
        for j in range(GROUP):
            q_rows[pl.ds(GROUP * e + j, ROWS, stride=HEADS), :] = block[:, D * j:D * (j + 1)]

    k_load.wait()
    v_load.wait()
    lane = lax.broadcasted_iota(jnp.int32, (HEADS, D), 1)
    head = lax.broadcasted_iota(jnp.int32, (HEADS, D), 0)
    same_kv = lax.rem(lane, KV) == head // GROUP
    step = lane // KV
    blocks = SEQ * KV // D
    per_block = D // KV

    def x_copy(b):
        return pltpu.make_async_remote_copy(part_send.at[b], part_recv.at[b], send_x.at[b], recv_x.at[b],
                                            device_id=dev(0, 1), device_id_type=MESH)

    for b in range(ROWS):
        q = q_rows[HEADS * b:HEADS * (b + 1), :].astype(BF16)
        s = lax.dot_general(q, kbuf[b].reshape(SEQ * KV, D), (((1,), (1,)), ((), ())), preferred_element_type=F32)
        limit = pos_smem[b] - core * SEQ
        tiles = [jnp.where(same_kv & (step < limit - per_block * j), s[:, D * j:D * (j + 1)], NEG)
                 for j in range(blocks)]
        top = functools.reduce(jnp.maximum, tiles)
        top = jnp.max(top, axis=1, keepdims=True)
        tiles = [jnp.exp2((t - top) * EXP2_SCALE) for t in tiles]
        total = jnp.sum(functools.reduce(jnp.add, tiles), axis=1, keepdims=True)
        p = jnp.concatenate([t.astype(BF16) for t in tiles], axis=1)
        acc = jnp.dot(p, vbuf[b].reshape(SEQ * KV, D), preferred_element_type=F32)
        rows = slice(MY * b, MY * (b + 1))
        for i, v in enumerate((acc, jnp.broadcast_to(top, (HEADS, D)), jnp.broadcast_to(total, (HEADS, D)))):
            low, high = v[0:MY], v[MY:HEADS]
            part_send[b, i] = jnp.where(core == 0, high, low)
            part_own[i, rows, :] = jnp.where(core == 0, low, high)
        x_copy(b).start()

    for i in range(KV // 2):
        block = proj_recv[core * (KV // 2) + i].astype(F32)
        for j in range(GROUP):
            at = pl.ds(GROUP * i + j, ROWS, stride=MY)
            k_exp[at, :] = block[:, QCOLS:QCOLS + D]
            v_exp[at, :] = block[:, QCOLS + D:]
    q_mine = jnp.concatenate([q_rows[pl.ds(pl.multiple_of(HEADS * b + MY * core, 8), MY), :] for b in range(ROWS)], axis=0)
    s_new = jnp.sum(q_mine * k_exp[...], axis=1, keepdims=True)

    for b in range(ROWS):
        x_copy(b).wait_recv()
    peer = [part_recv[:, i].reshape(ROWS * MY, D) for i in range(3)]
    top = jnp.maximum(jnp.maximum(part_own[1], peer[1]), s_new)
    w_own = jnp.exp2((part_own[1] - top) * EXP2_SCALE)
    w_peer = jnp.exp2((peer[1] - top) * EXP2_SCALE)
    w_new = jnp.exp2((s_new - top) * EXP2_SCALE)
    total = part_own[2] * w_own + peer[2] * w_peer + w_new
    o_rows[...] = (part_own[0] * w_own + peer[0] * w_peer + v_exp[...] * w_new) / total

    o_lhs[...] = jnp.zeros_like(o_lhs)
    for h in range(MY):
        o_lhs[0:ROWS, D * h:D * (h + 1)] = o_rows[pl.ds(h, ROWS, stride=MY), :]
    o_bf = o_lhs[...].astype(BF16)

    def p_copy(n):
        return pltpu.make_async_remote_copy(out_send.at[n], out_recv.at[n], send_p.at[n], recv_p.at[n],
                                            device_id=dev(0, 1), device_id_type=MESH)

    def out_body(n, _):
        wo_copy(n).wait()
        out_send[n] = jnp.dot(o_bf, w_o[n], preferred_element_type=F32)[0:ROWS]
        p_copy(n).start()
        return 0

    lax.fori_loop(0, NOUT, out_body, 0)

    tick = (lax.broadcasted_iota(jnp.int32, (16, 16, D), 0) * 2
            + lax.broadcasted_iota(jnp.int32, (16, 16, D), 1) // KV).astype(F32).astype(BF16)
    for b in range(ROWS):
        at = pos_smem[b] - core * SEQ
        for buf, off in ((kbuf, QCOLS), (vbuf, QCOLS + D)):
            new = jnp.concatenate([proj_recv[e][b:b + 1, off:off + D].astype(F32) for e in range(KV)] * 2, axis=0)
            new = new.astype(BF16)

            def put(i, _):
                want = (at - i * 32).astype(F32).astype(BF16)
                rows = pl.ds(pl.multiple_of(i * 16, 16), 16)
                buf[b, rows] = jnp.where(tick == want, new[None], buf[b, rows])
                return 0
            lax.fori_loop(0, SEQ // 32, put, 0)
    k_store = pltpu.make_async_copy(kbuf, k_next, sem_out.at[0])
    v_store = pltpu.make_async_copy(vbuf, v_next, sem_out.at[1])
    k_store.start()
    v_store.start()

    for n in range(NOUT):
        p_copy(n).wait_recv()
        attn_out[:, NCH * n:NCH * (n + 1)] = (out_send[n] + out_recv[n]).astype(BF16)

    for r in (1, 2, 3):
        a_copy(r).wait_send()
        f_copy(r).wait_send()
    for r, d in peers:
        b_copy(r, d, mine).wait_send()
    for b in range(ROWS):
        x_copy(b).wait_send()
    for n in range(NOUT):
        p_copy(n).wait_send()
    k_store.wait()
    v_store.wait()


def solution(mesh):
    row_spec = P(('rep', 'dp'), None)
    cache_spec = P(('rep', 'dp'), 'sp', None, None)
    len_spec = P(('rep', 'dp'))
    y_stride = 4 if mesh.shape['dp'] >= 8 else 2

    def local_step(hidden, w_query, w_key, w_value, w_out, k_cache, v_cache, write_pos, valid_len):
        shape = k_cache.shape
        pairs = (ROWS, SEQ * KV // 16, 16, D)
        any_spec = pl.BlockSpec(memory_space=pl.ANY)
        vmem = pltpu.VMEM
        dma = pltpu.SemaphoreType.DMA
        attn_out, k_next, v_next = pl.pallas_call(
            functools.partial(step_kernel, y_stride),
            out_shape=[jax.ShapeDtypeStruct(hidden.shape, BF16),
                       jax.ShapeDtypeStruct(pairs, BF16), jax.ShapeDtypeStruct(pairs, BF16)],
            in_specs=[any_spec] * 8,
            out_specs=[pl.BlockSpec(memory_space=vmem), any_spec, any_spec],
            scratch_shapes=[
                pltpu.SMEM((ROWS,), jnp.int32),
                vmem((CHIPS, 2, ROWS, HALF), BF16),
                vmem((2, CHIPS * ROWS, HALF), F32),
                vmem((WIDTH, COLS), BF16),
                vmem((CHIPS * ROWS, COLS), F32),
                vmem((CHIPS, ROWS, COLS), BF16),
                vmem((KV, ROWS, COLS), BF16),
                vmem((ROWS * HEADS, D), F32),
                vmem(pairs, BF16),
                vmem(pairs, BF16),
                vmem((NOUT, HALF, NCH), BF16),
                vmem((ROWS, 3, MY, D), F32),
                vmem((ROWS, 3, MY, D), F32),
                vmem((3, ROWS * MY, D), F32),
                vmem((ROWS * MY, D), F32),
                vmem((ROWS * MY, D), F32),
                vmem((ROWS * MY, D), F32),
                vmem((16, HALF), F32),
                vmem((NOUT, ROWS, NCH), F32),
                vmem((NOUT, ROWS, NCH), F32),
                dma((3,)), dma((WIDTH // KCH, 3)), dma((2,)), dma((NOUT,)),
                dma((CHIPS,)), dma((CHIPS,)), dma((CHIPS,)), dma((CHIPS,)),
                dma((CHIPS, 2)), dma((KV,)),
                dma((ROWS,)), dma((ROWS,)), dma((NOUT,)), dma((NOUT,)), dma((2,)),
            ],
            compiler_params=pltpu.CompilerParams(
                collective_id=0, has_side_effects=True, vmem_limit_bytes=62 * 1024 * 1024),
            cost_estimate=pl.CostEstimate(flops=10 ** 9, bytes_accessed=6 * 10 ** 7, transcendentals=10 ** 6),
        )(hidden, w_query, w_key, w_value, w_out, k_cache.reshape(pairs), v_cache.reshape(pairs), write_pos)
        return attn_out, k_next.reshape(shape), v_next.reshape(shape)

    return jax.shard_map(local_step, mesh=mesh, in_specs=(row_spec, P(), P(), P(), P('sp', None), cache_spec, cache_spec, len_spec, len_spec), out_specs=(row_spec, cache_spec, cache_spec), check_vma=False)
```

```python
import functools

import jax
import jax.numpy as jnp
from jax import lax
from jax.experimental import pallas as pl
from jax.experimental.pallas import tpu as pltpu
from jax.sharding import PartitionSpec as P

MESH = pl.DeviceIdType.MESH
BF16, F32 = jnp.bfloat16, jnp.float32

ROWS = 4
CHIPS = 4
D = 128
KV = 8
GROUP = 6
HEADS = KV * GROUP
WIDTH = 6144
HALF = WIDTH // 2
COLS = (GROUP + 2) * D
QCOLS = GROUP * D
SEQ = 256
MY = HEADS // 2
KCH = 3072
NCH = 1024
NBIG = 1024
NWO = WIDTH // NBIG
NOUT = WIDTH // NCH
NEG = -1e30
EXP2_SCALE = D ** -0.5 * 1.4426950408889634


def step_kernel(y_stride, hidden, w_query, w_key, w_value, w_out, k_cache, v_cache, write_pos,
                attn_out, kbuf, vbuf,
                pos_smem, gather, x32, w_in, proj, proj_send, proj_recv, q_rows, w_o,
                part_send, part_recv, part_own, k_exp, v_exp, kv_rows, o_rows, o_lhs, out_send, out_recv,
                sem_misc, sem_w, sem_kv, sem_wo, send_a, recv_a, send_f, recv_f, send_b, recv_b,
                send_x, recv_x, send_p, recv_p):
    core = lax.axis_index('sp')
    other = 1 - core
    dp = lax.axis_index('dp')
    xb = lax.rem(dp, 2)
    yb = lax.rem(dp // y_stride, 2)
    dx, dy = 1 - 2 * xb, 1 - 2 * yb
    chip = [dp, dp + dx, dp + y_stride * dy, dp + dx + y_stride * dy]
    spot0 = xb + 2 * yb
    spot = [spot0, spot0 + dx, spot0 + 2 * dy, spot0 + dx + 2 * dy]
    cores = [core, other]
    mine = spot0 * 2 + core

    def dev(r, d):
        return {'dp': chip[r], 'sp': cores[d]}

    peers = [(3, 0), (3, 1), (1, 0), (1, 1), (2, 0), (2, 1), (0, 1)]

    own = [pltpu.make_async_copy(hidden.at[:, pl.ds(h * HALF, HALF)], gather.at[0, h], sem_misc.at[h])
           for h in range(2)]
    pos_copy = pltpu.make_async_copy(write_pos, pos_smem, sem_misc.at[2])
    for cp in (*own, pos_copy):
        cp.start()

    col_q = pl.ds(pl.multiple_of(mine * QCOLS, D), QCOLS)
    col_k = pl.ds(pl.multiple_of(mine * D, D), D)
    w_loads = [pltpu.make_async_copy(w_query.at[:, col_q], w_in.at[:, pl.ds(0, QCOLS)], sem_w.at[0]),
               pltpu.make_async_copy(w_key.at[:, col_k], w_in.at[:, pl.ds(QCOLS, D)], sem_w.at[1]),
               pltpu.make_async_copy(w_value.at[:, col_k], w_in.at[:, pl.ds(QCOLS + D, D)], sem_w.at[2])]

    barrier = pltpu.get_barrier_semaphore()
    for r, d in peers:
        pl.semaphore_signal(barrier, inc=1, device_id=dev(r, d), device_id_type=MESH)
    for cp in own:
        cp.wait()
    for cp in w_loads:
        cp.start()
    for h in range(2):
        x32[h, 0:ROWS, :] = gather[0, h].astype(F32)
    pl.semaphore_wait(barrier, len(peers))

    def a_copy(r):
        return pltpu.make_async_remote_copy(gather.at[0, core], gather.at[r, core], send_a.at[r], recv_a.at[r],
                                            device_id=dev(r, 0), device_id_type=MESH)

    def f_copy(r):
        return pltpu.make_async_remote_copy(gather.at[r, core], gather.at[r, core], send_f.at[r], recv_f.at[r],
                                            device_id=dev(0, 1), device_id_type=MESH)

    for r in (3, 1, 2):
        a_copy(r).start()

    k_load = pltpu.make_async_copy(k_cache, kbuf, sem_kv.at[0])
    v_load = pltpu.make_async_copy(v_cache, vbuf, sem_kv.at[1])

    def wo_copy(n):
        return pltpu.make_async_copy(w_out.at[:, pl.ds(pl.multiple_of(n * NBIG, NBIG), NBIG)], w_o.at[n], sem_wo.at[n])

    for r in (1, 2, 3):
        a_copy(r).wait_recv()
        f_copy(r).start()
        if r == 1:
            for cp in (k_load, v_load, wo_copy(0), wo_copy(1)):
                cp.start()
        x32[core, ROWS * r:ROWS * (r + 1), :] = gather[r, core].astype(F32)

    def project(half):
        def body(i, _):
            k = half * per_half + i
            x = x32[half, :, pl.ds(pl.multiple_of(i * KCH, KCH), KCH)].astype(BF16)
            w = w_in[pl.ds(pl.multiple_of(k * KCH, KCH), KCH), :]
            proj[...] += jnp.dot(x, w, preferred_element_type=F32)
            return 0
        lax.fori_loop(0, per_half, body, 0)

    per_half = HALF // KCH
    proj[...] = jnp.zeros_like(proj)
    for cp in w_loads:
        cp.wait()
    project(core)
    for r in (1, 2, 3):
        f_copy(r).wait_recv()
        x32[other, ROWS * r:ROWS * (r + 1), :] = gather[r, other].astype(F32)
    project(other)
    wo_copy(2).start()
    wo_copy(3).start()

    for r in range(CHIPS):
        proj_send[r] = proj[ROWS * r:ROWS * (r + 1), :].astype(BF16)

    def b_copy(r, d, slot):
        return pltpu.make_async_remote_copy(proj_send.at[r], proj_recv.at[slot], send_b.at[r, d], recv_b.at[slot],
                                            device_id=dev(r, d), device_id_type=MESH)

    for r, d in peers:
        b_copy(r, d, mine).start()
    proj_recv[mine] = proj_send[0]
    pos_copy.wait()
    for r, d in peers:
        b_copy(r, d, spot[r] * 2 + cores[d]).wait_recv()

    for e in range(KV):
        block = proj_recv[e].astype(F32)
        for j in range(GROUP):
            q_rows[pl.ds(GROUP * e + j, ROWS, stride=HEADS), :] = block[:, D * j:D * (j + 1)]

    wo_copy(4).start()
    wo_copy(5).start()
    k_load.wait()
    v_load.wait()
    lane = lax.broadcasted_iota(jnp.int32, (HEADS, D), 1)
    head = lax.broadcasted_iota(jnp.int32, (HEADS, D), 0)
    same_kv = lax.rem(lane, KV) == head // GROUP
    step = lane // KV
    blocks = SEQ * KV // D
    per_block = D // KV

    def x_copy(b):
        return pltpu.make_async_remote_copy(part_send.at[b], part_recv.at[b], send_x.at[b], recv_x.at[b],
                                            device_id=dev(0, 1), device_id_type=MESH)

    def scores(b):
        q = q_rows[HEADS * b:HEADS * (b + 1), :].astype(BF16)
        return lax.dot_general(q, kbuf[b].reshape(SEQ * KV, D), (((1,), (1,)), ((), ())), preferred_element_type=F32)

    def soften(b, s):
        limit = pos_smem[b] - core * SEQ
        tiles = [jnp.where(same_kv & (step < limit - per_block * j), s[:, D * j:D * (j + 1)], NEG)
                 for j in range(blocks)]
        top = functools.reduce(jnp.maximum, tiles)
        top = jnp.max(top, axis=1, keepdims=True)
        tiles = [jnp.exp2((t - top) * EXP2_SCALE) for t in tiles]
        total = jnp.sum(functools.reduce(jnp.add, tiles), axis=1, keepdims=True)
        return top, total, jnp.concatenate([t.astype(BF16) for t in tiles], axis=1)

    def values(b, top, total, p):
        acc = jnp.dot(p, vbuf[b].reshape(SEQ * KV, D), preferred_element_type=F32)
        rows = slice(MY * b, MY * (b + 1))
        for i, v in enumerate((acc, jnp.broadcast_to(top, (HEADS, D)), jnp.broadcast_to(total, (HEADS, D)))):
            low, high = v[0:MY], v[MY:HEADS]
            part_send[b, i] = jnp.where(core == 0, high, low)
            part_own[i, rows, :] = jnp.where(core == 0, low, high)
        x_copy(b).start()

    raw = [scores(b) for b in range(ROWS)]
    soft = [soften(b, raw[b]) for b in range(ROWS)]
    for b in range(ROWS):
        values(b, *soft[b])
    for i in range(KV // 2):
        block = proj_recv[core * (KV // 2) + i].astype(F32)
        for j in range(GROUP):
            at = pl.ds(GROUP * i + j, ROWS, stride=MY)
            k_exp[at, :] = block[:, QCOLS:QCOLS + D]
            v_exp[at, :] = block[:, QCOLS + D:]
    for e in range(KV):
        block = proj_recv[e].astype(F32)
        for i in range(2):
            for at in (e, e + KV):
                kv_rows[i, pl.ds(at, ROWS, stride=2 * KV), :] = block[:, QCOLS + D * i:QCOLS + D * (i + 1)]
    q_mine = jnp.concatenate([q_rows[pl.ds(pl.multiple_of(HEADS * b + MY * core, 8), MY), :] for b in range(ROWS)], axis=0)
    s_new = jnp.sum(q_mine * k_exp[...], axis=1, keepdims=True)

    tick = (lax.broadcasted_iota(jnp.int32, (16, 16, D), 0) * 2
            + lax.broadcasted_iota(jnp.int32, (16, 16, D), 1) // KV).astype(F32).astype(BF16)

    def put(which, buf):
        def body(i, _):
            rows = pl.ds(pl.multiple_of(i * 16, 16), 16)
            for b in range(ROWS):
                want = (pos_smem[b] - core * SEQ - i * 32).astype(F32).astype(BF16)
                new = kv_rows[which, 2 * KV * b:2 * KV * (b + 1), :].astype(BF16)
                buf[b, rows] = jnp.where(tick == want, new[None], buf[b, rows])
            return 0
        lax.fori_loop(0, SEQ // 32, body, 0)

    put(0, kbuf)

    for b in range(ROWS):
        x_copy(b).wait_recv()
    peer = [part_recv[:, i].reshape(ROWS * MY, D) for i in range(3)]
    top = jnp.maximum(jnp.maximum(part_own[1], peer[1]), s_new)
    w_own = jnp.exp2((part_own[1] - top) * EXP2_SCALE)
    w_peer = jnp.exp2((peer[1] - top) * EXP2_SCALE)
    w_new = jnp.exp2((s_new - top) * EXP2_SCALE)
    total = part_own[2] * w_own + peer[2] * w_peer + w_new
    o_rows[...] = (part_own[0] * w_own + peer[0] * w_peer + v_exp[...] * w_new) / total

    o_lhs[...] = jnp.zeros_like(o_lhs)
    for h in range(MY):
        o_lhs[0:ROWS, D * h:D * (h + 1)] = o_rows[pl.ds(h, ROWS, stride=MY), :]
    o_bf = o_lhs[...].astype(BF16)

    def p_copy(n):
        return pltpu.make_async_remote_copy(out_send.at[n], out_recv.at[n], send_p.at[n], recv_p.at[n],
                                            device_id=dev(0, 1), device_id_type=MESH)

    for big in range(NWO):
        wo_copy(big).wait()
        for sub in range(NBIG // NCH):
            n = big * (NBIG // NCH) + sub
            out_send[n] = jnp.dot(o_bf, w_o[big, :, NCH * sub:NCH * (sub + 1)], preferred_element_type=F32)[0:ROWS]
            p_copy(n).start()

    put(1, vbuf)
    for n in range(NOUT):
        p_copy(n).wait_recv()
        attn_out[:, NCH * n:NCH * (n + 1)] = (out_send[n] + out_recv[n]).astype(BF16)

    for r in (1, 2, 3):
        a_copy(r).wait_send()
        f_copy(r).wait_send()
    for r, d in peers:
        b_copy(r, d, mine).wait_send()
    for b in range(ROWS):
        x_copy(b).wait_send()
    for n in range(NOUT):
        p_copy(n).wait_send()


def finish_kernel(attn, k_old, v_old, attn_out, k_next, v_next, sem):
    copies = [pltpu.make_async_copy(src, dst, sem.at[i])
              for i, (src, dst) in enumerate(((k_old, k_next), (v_old, v_next), (attn, attn_out)))]
    for cp in copies:
        cp.start()
    for cp in copies:
        cp.wait()


def solution(mesh):
    row_spec = P(('rep', 'dp'), None)
    cache_spec = P(('rep', 'dp'), 'sp', None, None)
    len_spec = P(('rep', 'dp'))
    y_stride = 4 if mesh.shape['dp'] >= 8 else 2

    def local_step(hidden, w_query, w_key, w_value, w_out, k_cache, v_cache, write_pos, valid_len):
        shape = k_cache.shape
        pairs = (ROWS, SEQ * KV // 16, 16, D)
        any_spec = pl.BlockSpec(memory_space=pl.ANY)
        vmem = pltpu.VMEM
        dma = pltpu.SemaphoreType.DMA
        attn, k_old, v_old = pl.pallas_call(
            functools.partial(step_kernel, y_stride),
            out_shape=[vmem(hidden.shape, BF16), vmem(pairs, BF16), vmem(pairs, BF16)],
            in_specs=[any_spec] * 8,
            out_specs=[pl.BlockSpec(memory_space=vmem)] * 3,
            scratch_shapes=[
                pltpu.SMEM((ROWS,), jnp.int32),
                vmem((CHIPS, 2, ROWS, HALF), BF16),
                vmem((2, CHIPS * ROWS, HALF), F32),
                vmem((WIDTH, COLS), BF16),
                vmem((CHIPS * ROWS, COLS), F32),
                vmem((CHIPS, ROWS, COLS), BF16),
                vmem((KV, ROWS, COLS), BF16),
                vmem((ROWS * HEADS, D), F32),
                vmem((NWO, HALF, NBIG), BF16),
                vmem((ROWS, 3, MY, D), F32),
                vmem((ROWS, 3, MY, D), F32),
                vmem((3, ROWS * MY, D), F32),
                vmem((ROWS * MY, D), F32),
                vmem((ROWS * MY, D), F32),
                vmem((2, ROWS * 2 * KV, D), F32),
                vmem((ROWS * MY, D), F32),
                vmem((16, HALF), F32),
                vmem((NOUT, ROWS, NCH), F32),
                vmem((NOUT, ROWS, NCH), F32),
                dma((3,)), dma((3,)), dma((2,)), dma((NWO,)),
                dma((CHIPS,)), dma((CHIPS,)), dma((CHIPS,)), dma((CHIPS,)),
                dma((CHIPS, 2)), dma((KV,)),
                dma((ROWS,)), dma((ROWS,)), dma((NOUT,)), dma((NOUT,)),
            ],
            compiler_params=pltpu.CompilerParams(
                collective_id=0, has_side_effects=True, vmem_limit_bytes=54 * 1024 * 1024),
            cost_estimate=pl.CostEstimate(flops=10 ** 9, bytes_accessed=6 * 10 ** 7, transcendentals=10 ** 6),
        )(hidden, w_query, w_key, w_value, w_out, k_cache.reshape(pairs), v_cache.reshape(pairs), write_pos)
        return pl.pallas_call(
            finish_kernel,
            out_shape=[jax.ShapeDtypeStruct(hidden.shape, BF16)] + [jax.ShapeDtypeStruct(shape, BF16)] * 2,
            in_specs=[any_spec] * 3,
            out_specs=[any_spec] * 3,
            scratch_shapes=[dma((3,))],
            compiler_params=pltpu.CompilerParams(vmem_limit_bytes=1024 * 1024),
            cost_estimate=pl.CostEstimate(flops=10 ** 6, bytes_accessed=10 ** 7, transcendentals=0),
        )(attn, k_old.reshape(shape), v_old.reshape(shape))

    return jax.shard_map(local_step, mesh=mesh, in_specs=(row_spec, P(), P(), P(), P('sp', None), cache_spec, cache_spec, len_spec, len_spec), out_specs=(row_spec, cache_spec, cache_spec), check_vma=False)
```

```python
import functools

import jax
import jax.numpy as jnp
from jax import lax
from jax.experimental import pallas as pl
from jax.experimental.pallas import tpu as pltpu
from jax.sharding import PartitionSpec as P

MESH = pl.DeviceIdType.MESH
BF16, F32 = jnp.bfloat16, jnp.float32

ROWS = 4
CHIPS = 4
D = 128
KV = 8
GROUP = 6
HEADS = KV * GROUP
WIDTH = 6144
HALF = WIDTH // 2
COLS = (GROUP + 2) * D
QCOLS = GROUP * D
SEQ = 256
MY = HEADS // 2
KCH = 3072
OUT_PARTS = [(0, 2048), (2048, 2048), (4096, 2048)]
NEG = -1e30
EXP2_SCALE = D ** -0.5 * 1.4426950408889634


def step_kernel(y_stride, hidden, w_query, w_key, w_value, w_out, k_cache, v_cache, write_pos,
                attn_out, kbuf, vbuf,
                pos_smem, gather, x32, w_in, proj, proj_send, proj_recv, q_rows, k_turned, w_o,
                part_send, part_recv, part_own, k_exp, v_exp, kv_rows, o_rows, o_lhs, out_send, out_recv,
                sem_misc, sem_w, sem_kv, sem_wo, send_a, recv_a, send_f, recv_f, send_b, recv_b,
                send_x, recv_x, send_p, recv_p):
    core = lax.axis_index('sp')
    other = 1 - core
    dp = lax.axis_index('dp')
    xb = lax.rem(dp, 2)
    yb = lax.rem(dp // y_stride, 2)
    dx, dy = 1 - 2 * xb, 1 - 2 * yb
    chip = [dp, dp + dx, dp + y_stride * dy, dp + dx + y_stride * dy]
    spot0 = xb + 2 * yb
    spot = [spot0, spot0 + dx, spot0 + 2 * dy, spot0 + dx + 2 * dy]
    cores = [core, other]
    mine = spot0 * 2 + core

    def dev(r, d):
        return {'dp': chip[r], 'sp': cores[d]}

    peers = [(3, 0), (3, 1), (1, 0), (1, 1), (2, 0), (2, 1), (0, 1)]

    col_q = pl.ds(pl.multiple_of(mine * QCOLS, D), QCOLS)
    col_k = pl.ds(pl.multiple_of(mine * D, D), D)
    q_load = pltpu.make_async_copy(w_query.at[:, col_q], w_in.at[:, pl.ds(0, QCOLS)], sem_w)
    kv_loads = [pltpu.make_async_copy(src.at[:, col_k], w_in.at[:, pl.ds(QCOLS + D * i, D)], sem_w)
                for i, src in enumerate((w_key, w_value))]

    def wo_copy(n):
        cols = pl.ds(OUT_PARTS[n][0], OUT_PARTS[n][1])
        return pltpu.make_async_copy(w_out.at[:, cols], w_o.at[:, cols], sem_wo.at[n])

    k_load = pltpu.make_async_copy(k_cache, kbuf, sem_kv.at[0])
    v_load = pltpu.make_async_copy(v_cache, vbuf, sem_kv.at[1])

    own = [pltpu.make_async_copy(hidden.at[:, pl.ds(h * HALF, HALF)], gather.at[0, h], sem_misc.at[h])
           for h in range(2)]
    pos_copy = pltpu.make_async_copy(write_pos, pos_smem, sem_misc.at[2])
    for cp in (*own, pos_copy, *kv_loads):
        cp.start()

    barrier = pltpu.get_barrier_semaphore()
    for r, d in peers:
        pl.semaphore_signal(barrier, inc=1, device_id=dev(r, d), device_id_type=MESH)
    for cp in own:
        cp.wait()
    q_load.start()
    for n in range(len(OUT_PARTS)):
        wo_copy(n).start(priority=1)
    for h in range(2):
        x32[h, 0:ROWS, :] = gather[0, h].astype(F32)
    pl.semaphore_wait(barrier, len(peers))

    def a_copy(r):
        return pltpu.make_async_remote_copy(gather.at[0, core], gather.at[r, core], send_a, recv_a.at[r - 1],
                                            device_id=dev(r, 0), device_id_type=MESH)

    def f_copy(r):
        return pltpu.make_async_remote_copy(gather.at[r, core], gather.at[r, core], send_f, recv_f,
                                            device_id=dev(0, 1), device_id_type=MESH)

    def whole(ref, send, recv):
        return pltpu.make_async_remote_copy(ref, ref, send, recv, device_id=dev(0, 1), device_id_type=MESH)

    for r in (3, 1, 2):
        a_copy(r).start()


    for r in (1, 2, 3):
        a_copy(r).wait_recv()
        f_copy(r).start()
        if r == 1:
            for cp in (k_load, v_load):
                cp.start()
        x32[core, ROWS * r:ROWS * (r + 1), :] = gather[r, core].astype(F32)

    def project(half):
        def body(i, _):
            k = half * per_half + i
            x = x32[half, :, pl.ds(pl.multiple_of(i * KCH, KCH), KCH)].astype(BF16)
            w = w_in[pl.ds(pl.multiple_of(k * KCH, KCH), KCH), :]
            proj[...] += jnp.dot(x, w, preferred_element_type=F32)
            return 0
        lax.fori_loop(0, per_half, body, 0)

    per_half = HALF // KCH
    proj[...] = jnp.zeros_like(proj)
    pltpu.make_async_copy(w_in, w_in, sem_w).wait()
    project(core)
    whole(gather.at[1:CHIPS, other], send_f, recv_f).wait_recv()
    for r in (1, 2, 3):
        x32[other, ROWS * r:ROWS * (r + 1), :] = gather[r, other].astype(F32)
    project(other)

    for r in range(CHIPS):
        proj_send[r] = proj[ROWS * r:ROWS * (r + 1), :].astype(BF16)

    def b_copy(r, d):
        return pltpu.make_async_remote_copy(proj_send.at[r], proj_recv.at[mine], send_b, recv_b,
                                            device_id=dev(r, d), device_id_type=MESH)

    for r, d in peers:
        b_copy(r, d).start()
    proj_recv[mine] = proj_send[0]
    k_load.wait()
    for b in range(ROWS):
        k_turned[b] = kbuf[b].reshape(SEQ * KV, D).T
    pos_copy.wait()
    whole(proj_recv.at[0:len(peers)], send_b, recv_b).wait_recv()

    for e in range(KV):
        block = proj_recv[e].astype(F32)
        for j in range(GROUP):
            q_rows[pl.ds(GROUP * e + j, ROWS, stride=HEADS), :] = block[:, D * j:D * (j + 1)]

    v_load.wait()
    lane = lax.broadcasted_iota(jnp.int32, (HEADS, D), 1)
    head = lax.broadcasted_iota(jnp.int32, (HEADS, D), 0)
    same_kv = lax.rem(lane, KV) == head // GROUP
    step = lane // KV
    blocks = SEQ * KV // D
    per_block = D // KV

    def scores(b):
        q = q_rows[HEADS * b:HEADS * (b + 1), :].astype(BF16)
        return jnp.dot(q, k_turned[b], preferred_element_type=F32)

    def soften(b, s):
        limit = pos_smem[b] - core * SEQ
        tiles = [jnp.where(same_kv & (step < limit - per_block * j), s[:, D * j:D * (j + 1)], NEG)
                 for j in range(blocks)]
        top = functools.reduce(jnp.maximum, tiles)
        top = jnp.max(top, axis=1, keepdims=True)
        tiles = [jnp.exp2((t - top) * EXP2_SCALE) for t in tiles]
        total = jnp.sum(functools.reduce(jnp.add, tiles), axis=1, keepdims=True)
        return top, total, jnp.concatenate([t.astype(BF16) for t in tiles], axis=1)

    def values(b, top, total, p):
        acc = jnp.dot(p, vbuf[b].reshape(SEQ * KV, D), preferred_element_type=F32)
        rows = slice(MY * b, MY * (b + 1))
        for i, v in enumerate((acc, jnp.broadcast_to(top, (HEADS, D)), jnp.broadcast_to(total, (HEADS, D)))):
            low, high = v[0:MY], v[MY:HEADS]
            part_send[b, i] = jnp.where(core == 0, high, low)
            part_own[i, rows, :] = jnp.where(core == 0, low, high)

    raw = [scores(b) for b in range(ROWS)]
    soft = [soften(b, raw[b]) for b in range(ROWS)]
    for b in range(ROWS):
        values(b, *soft[b])
    x_copy = pltpu.make_async_remote_copy(part_send, part_recv, send_x, recv_x,
                                          device_id=dev(0, 1), device_id_type=MESH)
    x_copy.start()

    for i in range(KV // 2):
        block = proj_recv[core * (KV // 2) + i].astype(F32)
        for j in range(GROUP):
            at = pl.ds(GROUP * i + j, ROWS, stride=MY)
            k_exp[at, :] = block[:, QCOLS:QCOLS + D]
            v_exp[at, :] = block[:, QCOLS + D:]
    for e in range(KV):
        block = proj_recv[e].astype(F32)
        for i in range(2):
            for at in (e, e + KV):
                kv_rows[i, pl.ds(at, ROWS, stride=2 * KV), :] = block[:, QCOLS + D * i:QCOLS + D * (i + 1)]
    q_mine = jnp.concatenate([q_rows[pl.ds(pl.multiple_of(HEADS * b + MY * core, 8), MY), :] for b in range(ROWS)], axis=0)
    s_new = jnp.sum(q_mine * k_exp[...], axis=1, keepdims=True)

    tick = (lax.broadcasted_iota(jnp.int32, (16, 16, D), 0) * 2
            + lax.broadcasted_iota(jnp.int32, (16, 16, D), 1) // KV).astype(F32).astype(BF16)

    def put(which, buf):
        def body(i, _):
            rows = pl.ds(pl.multiple_of(i * 16, 16), 16)
            for b in range(ROWS):
                want = (pos_smem[b] - core * SEQ - i * 32).astype(F32).astype(BF16)
                new = kv_rows[which, 2 * KV * b:2 * KV * (b + 1), :].astype(BF16)
                buf[b, rows] = jnp.where(tick == want, new[None], buf[b, rows])
            return 0
        lax.fori_loop(0, SEQ // 32, body, 0)

    put(0, kbuf)

    x_copy.wait_recv()
    peer = [part_recv[:, i].reshape(ROWS * MY, D) for i in range(3)]
    top = jnp.maximum(jnp.maximum(part_own[1], peer[1]), s_new)
    w_own = jnp.exp2((part_own[1] - top) * EXP2_SCALE)
    w_peer = jnp.exp2((peer[1] - top) * EXP2_SCALE)
    w_new = jnp.exp2((s_new - top) * EXP2_SCALE)
    total = part_own[2] * w_own + peer[2] * w_peer + w_new
    o_rows[...] = (part_own[0] * w_own + peer[0] * w_peer + v_exp[...] * w_new) / total

    o_lhs[...] = jnp.zeros_like(o_lhs)
    for h in range(MY):
        o_lhs[0:ROWS, D * h:D * (h + 1)] = o_rows[pl.ds(h, ROWS, stride=MY), :]
    o_bf = o_lhs[...].astype(BF16)

    def p_copy(n):
        cols = pl.ds(OUT_PARTS[n][0], OUT_PARTS[n][1])
        return pltpu.make_async_remote_copy(out_send.at[:, cols], out_recv.at[:, cols], send_p, recv_p,
                                            device_id=dev(0, 1), device_id_type=MESH)

    for n, (at, width) in enumerate(OUT_PARTS):
        wo_copy(n).wait()
        out_send[:, at:at + width] = jnp.dot(o_bf, w_o[:, at:at + width], preferred_element_type=F32)[0:ROWS]
        p_copy(n).start()
    put(1, vbuf)
    whole(out_recv, send_p, recv_p).wait_recv()
    attn_out[...] = (out_send[...] + out_recv[...]).astype(BF16)

    whole(gather.at[1:CHIPS, core], send_a, recv_a.at[0]).wait_send()
    whole(gather.at[1:CHIPS, core], send_f, recv_f).wait_send()
    whole(proj_recv.at[0:len(peers)], send_b, recv_b).wait_send()
    x_copy.wait_send()
    whole(out_send, send_p, recv_p).wait_send()


def finish_kernel(attn, k_old, v_old, attn_out, k_next, v_next, sem):
    copies = [pltpu.make_async_copy(src, dst, sem.at[i])
              for i, (src, dst) in enumerate(((k_old, k_next), (v_old, v_next), (attn, attn_out)))]
    for cp in copies:
        cp.start()
    for cp in copies:
        cp.wait()


def solution(mesh):
    row_spec = P(('rep', 'dp'), None)
    cache_spec = P(('rep', 'dp'), 'sp', None, None)
    len_spec = P(('rep', 'dp'))
    y_stride = 4 if mesh.shape['dp'] >= 8 else 2

    def local_step(hidden, w_query, w_key, w_value, w_out, k_cache, v_cache, write_pos, valid_len):
        shape = k_cache.shape
        pairs = (ROWS, SEQ * KV // 16, 16, D)
        any_spec = pl.BlockSpec(memory_space=pl.ANY)
        vmem = pltpu.VMEM
        dma = pltpu.SemaphoreType.DMA
        attn, k_old, v_old = pl.pallas_call(
            functools.partial(step_kernel, y_stride),
            out_shape=[vmem(hidden.shape, BF16), vmem(pairs, BF16), vmem(pairs, BF16)],
            in_specs=[any_spec] * 8,
            out_specs=[pl.BlockSpec(memory_space=vmem)] * 3,
            scratch_shapes=[
                pltpu.SMEM((ROWS,), jnp.int32),
                vmem((CHIPS, 2, ROWS, HALF), BF16),
                vmem((2, CHIPS * ROWS, HALF), F32),
                vmem((WIDTH, COLS), BF16),
                vmem((CHIPS * ROWS, COLS), F32),
                vmem((CHIPS, ROWS, COLS), BF16),
                vmem((KV, ROWS, COLS), BF16),
                vmem((ROWS * HEADS, D), F32),
                vmem((ROWS, D, SEQ * KV), BF16),
                vmem((HALF, WIDTH), BF16),
                vmem((ROWS, 3, MY, D), F32),
                vmem((ROWS, 3, MY, D), F32),
                vmem((3, ROWS * MY, D), F32),
                vmem((ROWS * MY, D), F32),
                vmem((ROWS * MY, D), F32),
                vmem((2, ROWS * 2 * KV, D), F32),
                vmem((ROWS * MY, D), F32),
                vmem((16, HALF), F32),
                vmem((ROWS, WIDTH), F32),
                vmem((ROWS, WIDTH), F32),
                dma((3,)), dma, dma((2,)), dma((len(OUT_PARTS),)),
                dma, dma((CHIPS - 1,)), dma, dma, dma, dma, dma, dma, dma, dma,
            ],
            compiler_params=pltpu.CompilerParams(
                collective_id=0, has_side_effects=True, vmem_limit_bytes=56 * 1024 * 1024),
            cost_estimate=pl.CostEstimate(flops=10 ** 9, bytes_accessed=6 * 10 ** 7, transcendentals=10 ** 6),
        )(hidden, w_query, w_key, w_value, w_out, k_cache.reshape(pairs), v_cache.reshape(pairs), write_pos)
        return pl.pallas_call(
            finish_kernel,
            out_shape=[jax.ShapeDtypeStruct(hidden.shape, BF16)] + [jax.ShapeDtypeStruct(shape, BF16)] * 2,
            in_specs=[any_spec] * 3,
            out_specs=[any_spec] * 3,
            scratch_shapes=[dma((3,))],
            compiler_params=pltpu.CompilerParams(vmem_limit_bytes=1024 * 1024),
            cost_estimate=pl.CostEstimate(flops=10 ** 6, bytes_accessed=10 ** 7, transcendentals=0),
        )(attn, k_old.reshape(shape), v_old.reshape(shape))

    return jax.shard_map(local_step, mesh=mesh, in_specs=(row_spec, P(), P(), P(), P('sp', None), cache_spec, cache_spec, len_spec, len_spec), out_specs=(row_spec, cache_spec, cache_spec), check_vma=False)
```

```python
import functools

import jax
import jax.numpy as jnp
from jax import lax
from jax.experimental import pallas as pl
from jax.experimental.pallas import tpu as pltpu
from jax.sharding import PartitionSpec as P

MESH = pl.DeviceIdType.MESH
BF16, F32 = jnp.bfloat16, jnp.float32

ROWS = 4
CHIPS = 4
D = 128
KV = 8
GROUP = 6
HEADS = KV * GROUP
WIDTH = 6144
HALF = WIDTH // 2
COLS = (GROUP + 2) * D
QCOLS = GROUP * D
SEQ = 256
MY = HEADS // 2
OUT_PARTS = [(0, 2048), (2048, 2048), (4096, 1024), (5120, 1024)]
NEG = -1e30
EXP2_SCALE = D ** -0.5 * 1.4426950408889634


def step_kernel(y_stride, hidden, w_query, w_key, w_value, w_out, k_cache, v_cache, write_pos,
                attn_out, kbuf, vbuf,
                pos_smem, gather, x32, w_in, proj, proj_send, proj_recv, q_rows, k_turned, w_o,
                part_send, part_recv, part_own, k_exp, v_exp, kv_rows, o_rows, o_lhs, out_send, out_recv,
                sem_misc, sem_w, sem_kv, sem_wo, send_a, recv_a, send_f, recv_f, send_b, recv_b,
                send_x, recv_x, send_p, recv_p):
    core = lax.axis_index('sp')
    other = 1 - core
    dp = lax.axis_index('dp')
    xb = lax.rem(dp, 2)
    yb = lax.rem(dp // y_stride, 2)
    dx, dy = 1 - 2 * xb, 1 - 2 * yb
    chip = [dp, dp + dx, dp + y_stride * dy, dp + dx + y_stride * dy]
    spot0 = xb + 2 * yb
    spot = [spot0, spot0 + dx, spot0 + 2 * dy, spot0 + dx + 2 * dy]
    cores = [core, other]
    mine = spot0 * 2 + core

    def dev(r, d):
        return {'dp': chip[r], 'sp': cores[d]}

    peers = [(3, 0), (3, 1), (1, 0), (1, 1), (2, 0), (2, 1), (0, 1)]

    col_q = pl.ds(pl.multiple_of(mine * QCOLS, D), QCOLS)
    col_k = pl.ds(pl.multiple_of(mine * D, D), D)
    q_load = pltpu.make_async_copy(w_query.at[:, col_q], w_in.at[:, pl.ds(0, QCOLS)], sem_w)
    kv_loads = [pltpu.make_async_copy(src.at[:, col_k], w_in.at[:, pl.ds(QCOLS + D * i, D)], sem_w)
                for i, src in enumerate((w_key, w_value))]

    def wo_copy(n):
        cols = pl.ds(OUT_PARTS[n][0], OUT_PARTS[n][1])
        return pltpu.make_async_copy(w_out.at[:, cols], w_o.at[:, cols], sem_wo.at[n])

    k_load = pltpu.make_async_copy(k_cache, kbuf, sem_kv.at[0])
    v_load = pltpu.make_async_copy(v_cache, vbuf, sem_kv.at[1])

    own = [pltpu.make_async_copy(hidden.at[:, pl.ds(h * HALF, HALF)], gather.at[0, h], sem_misc.at[h])
           for h in range(2)]
    pos_copy = pltpu.make_async_copy(write_pos, pos_smem, sem_misc.at[2])
    for cp in (*own, pos_copy, *kv_loads):
        cp.start()

    barrier = pltpu.get_barrier_semaphore()
    for r, d in peers:
        pl.semaphore_signal(barrier, inc=1, device_id=dev(r, d), device_id_type=MESH)
    for cp in own:
        cp.wait()
    q_load.start()
    for n in range(len(OUT_PARTS)):
        wo_copy(n).start(priority=1)
    for h in range(2):
        x32[h, 0:ROWS, :] = gather[0, h].astype(F32)
    pl.semaphore_wait(barrier, len(peers))

    def a_copy(r):
        return pltpu.make_async_remote_copy(gather.at[0, core], gather.at[r, core], send_a, recv_a.at[r - 1],
                                            device_id=dev(r, 0), device_id_type=MESH)

    def f_copy(r):
        return pltpu.make_async_remote_copy(gather.at[r, core], gather.at[r, core], send_f, recv_f,
                                            device_id=dev(0, 1), device_id_type=MESH)

    def whole(ref, send, recv):
        return pltpu.make_async_remote_copy(ref, ref, send, recv, device_id=dev(0, 1), device_id_type=MESH)

    for r in (3, 1, 2):
        a_copy(r).start()


    for r in (1, 2, 3):
        a_copy(r).wait_recv()
        f_copy(r).start()
        if r == 1:
            for cp in (k_load, v_load):
                cp.start()
        x32[core, ROWS * r:ROWS * (r + 1), :] = gather[r, core].astype(F32)

    def project(half):
        rows = pl.ds(pl.multiple_of(half * HALF, HALF), HALF)
        return jnp.dot(x32[half].astype(BF16), w_in[rows, :], preferred_element_type=F32)

    pltpu.make_async_copy(w_in, w_in, sem_w).wait()
    proj[...] = project(core)
    whole(gather.at[1:CHIPS, other], send_f, recv_f).wait_recv()
    for r in (1, 2, 3):
        x32[other, ROWS * r:ROWS * (r + 1), :] = gather[r, other].astype(F32)
    done = (proj[...] + project(other)).astype(BF16)

    for r in range(CHIPS):
        proj_send[r] = done[ROWS * r:ROWS * (r + 1), :]

    def b_copy(r, d):
        return pltpu.make_async_remote_copy(proj_send.at[r], proj_recv.at[mine], send_b, recv_b,
                                            device_id=dev(r, d), device_id_type=MESH)

    for r, d in peers:
        b_copy(r, d).start()
    proj_recv[mine] = proj_send[0]
    k_load.wait()
    for b in range(ROWS):
        k_turned[b] = kbuf[b].reshape(SEQ * KV, D).T
    pos_copy.wait()
    whole(proj_recv.at[0:len(peers)], send_b, recv_b).wait_recv()

    for e in range(KV):
        block = proj_recv[e].astype(F32)
        for j in range(GROUP):
            q_rows[pl.ds(GROUP * e + j, ROWS, stride=HEADS), :] = block[:, D * j:D * (j + 1)]

    v_load.wait()
    lane = lax.broadcasted_iota(jnp.int32, (HEADS, D), 1)
    head = lax.broadcasted_iota(jnp.int32, (HEADS, D), 0)
    same_kv = lax.rem(lane, KV) == head // GROUP
    step = lane // KV
    stat_of = lane // (D // (2 * ROWS))
    blocks = SEQ * KV // D
    per_block = D // KV

    def scores(b):
        q = q_rows[HEADS * b:HEADS * (b + 1), :].astype(BF16)
        return jnp.dot(q, k_turned[b], preferred_element_type=F32)

    def soften(b, s):
        limit = pos_smem[b] - core * SEQ
        tiles = [jnp.where(same_kv & (step < limit - per_block * j), s[:, D * j:D * (j + 1)], NEG)
                 for j in range(blocks)]
        top = functools.reduce(jnp.maximum, tiles)
        top = jnp.max(top, axis=1, keepdims=True)
        tiles = [jnp.exp2((t - top) * EXP2_SCALE) for t in tiles]
        total = jnp.sum(functools.reduce(jnp.add, tiles), axis=1, keepdims=True)
        return top, total, jnp.concatenate([t.astype(BF16) for t in tiles], axis=1)

    def values(b, top, total, p):
        acc = jnp.dot(p, vbuf[b].reshape(SEQ * KV, D), preferred_element_type=F32)
        rows = slice(MY * b, MY * (b + 1))
        stats = jnp.where(stat_of == 2 * b, top, jnp.where(stat_of == 2 * b + 1, total, 0.0))
        part_send[b] = jnp.where(core == 0, acc[MY:HEADS], acc[0:MY])
        part_own[0, rows, :] = jnp.where(core == 0, acc[0:MY], acc[MY:HEADS])
        for i, v in enumerate((top, total)):
            part_own[1 + i, rows, :] = jnp.broadcast_to(jnp.where(core == 0, v[0:MY], v[MY:HEADS]), (MY, D))
        return stats

    raw = [scores(b) for b in range(ROWS)]
    soft = [soften(b, raw[b]) for b in range(ROWS)]
    stats = functools.reduce(jnp.add, [values(b, *soft[b]) for b in range(ROWS)])
    part_send[ROWS] = jnp.where(core == 0, stats[MY:HEADS], stats[0:MY])
    x_copy = pltpu.make_async_remote_copy(part_send, part_recv, send_x, recv_x,
                                          device_id=dev(0, 1), device_id_type=MESH)
    x_copy.start()

    for i in range(KV // 2):
        block = proj_recv[core * (KV // 2) + i].astype(F32)
        for j in range(GROUP):
            at = pl.ds(GROUP * i + j, ROWS, stride=MY)
            k_exp[at, :] = block[:, QCOLS:QCOLS + D]
            v_exp[at, :] = block[:, QCOLS + D:]
    for e in range(KV):
        block = proj_recv[e].astype(F32)
        for i in range(2):
            for at in (e, e + KV):
                kv_rows[i, pl.ds(at, ROWS, stride=2 * KV), :] = block[:, QCOLS + D * i:QCOLS + D * (i + 1)]
    q_mine = jnp.concatenate([q_rows[pl.ds(pl.multiple_of(HEADS * b + MY * core, 8), MY), :] for b in range(ROWS)], axis=0)
    s_new = jnp.sum(q_mine * k_exp[...], axis=1, keepdims=True)

    tick = (lax.broadcasted_iota(jnp.int32, (16, 16, D), 0) * 2
            + lax.broadcasted_iota(jnp.int32, (16, 16, D), 1) // KV).astype(F32).astype(BF16)

    def put(which, buf):
        def body(i, _):
            rows = pl.ds(pl.multiple_of(i * 16, 16), 16)
            for b in range(ROWS):
                want = (pos_smem[b] - core * SEQ - i * 32).astype(F32).astype(BF16)
                new = kv_rows[which, 2 * KV * b:2 * KV * (b + 1), :].astype(BF16)
                buf[b, rows] = jnp.where(tick == want, new[None], buf[b, rows])
            return 0
        lax.fori_loop(0, SEQ // 32, body, 0)

    put(0, kbuf)

    x_copy.wait_recv()
    stats = part_recv[ROWS]
    peer = [part_recv[0:ROWS].reshape(ROWS * MY, D)]
    for i in range(2):
        lanes = [D // (2 * ROWS) * (2 * b + i) for b in range(ROWS)]
        peer.append(jnp.concatenate([jnp.broadcast_to(stats[:, at:at + 1], (MY, D)) for at in lanes], axis=0))
    top = jnp.maximum(jnp.maximum(part_own[1], peer[1]), s_new)
    w_own = jnp.exp2((part_own[1] - top) * EXP2_SCALE)
    w_peer = jnp.exp2((peer[1] - top) * EXP2_SCALE)
    w_new = jnp.exp2((s_new - top) * EXP2_SCALE)
    total = part_own[2] * w_own + peer[2] * w_peer + w_new
    o_rows[...] = (part_own[0] * w_own + peer[0] * w_peer + v_exp[...] * w_new) / total

    o_lhs[...] = jnp.zeros_like(o_lhs)
    for h in range(MY):
        o_lhs[0:ROWS, D * h:D * (h + 1)] = o_rows[pl.ds(h, ROWS, stride=MY), :]
    o_bf = o_lhs[...].astype(BF16)

    def p_copy(n):
        cols = pl.ds(OUT_PARTS[n][0], OUT_PARTS[n][1])
        return pltpu.make_async_remote_copy(out_send.at[:, cols], out_recv.at[:, cols], send_p, recv_p,
                                            device_id=dev(0, 1), device_id_type=MESH)

    for n, (at, width) in enumerate(OUT_PARTS):
        wo_copy(n).wait()
        out_send[:, at:at + width] = jnp.dot(o_bf, w_o[:, at:at + width], preferred_element_type=F32)[0:ROWS]
        p_copy(n).start()
    put(1, vbuf)
    whole(out_recv, send_p, recv_p).wait_recv()
    attn_out[...] = (out_send[...] + out_recv[...]).astype(BF16)

    whole(gather.at[1:CHIPS, core], send_a, recv_a.at[0]).wait_send()
    whole(gather.at[1:CHIPS, core], send_f, recv_f).wait_send()
    whole(proj_recv.at[0:len(peers)], send_b, recv_b).wait_send()
    x_copy.wait_send()
    whole(out_send, send_p, recv_p).wait_send()


def finish_kernel(attn, k_old, v_old, attn_out, k_next, v_next, sem):
    copies = [pltpu.make_async_copy(src, dst, sem.at[i])
              for i, (src, dst) in enumerate(((k_old, k_next), (v_old, v_next), (attn, attn_out)))]
    for cp in copies:
        cp.start()
    for cp in copies:
        cp.wait()


def solution(mesh):
    row_spec = P(('rep', 'dp'), None)
    cache_spec = P(('rep', 'dp'), 'sp', None, None)
    len_spec = P(('rep', 'dp'))
    y_stride = 4 if mesh.shape['dp'] >= 8 else 2

    def local_step(hidden, w_query, w_key, w_value, w_out, k_cache, v_cache, write_pos, valid_len):
        shape = k_cache.shape
        pairs = (ROWS, SEQ * KV // 16, 16, D)
        any_spec = pl.BlockSpec(memory_space=pl.ANY)
        vmem = pltpu.VMEM
        dma = pltpu.SemaphoreType.DMA
        attn, k_old, v_old = pl.pallas_call(
            functools.partial(step_kernel, y_stride),
            out_shape=[vmem(hidden.shape, BF16), vmem(pairs, BF16), vmem(pairs, BF16)],
            in_specs=[any_spec] * 8,
            out_specs=[pl.BlockSpec(memory_space=vmem)] * 3,
            scratch_shapes=[
                pltpu.SMEM((ROWS,), jnp.int32),
                vmem((CHIPS, 2, ROWS, HALF), BF16),
                vmem((2, CHIPS * ROWS, HALF), F32),
                vmem((WIDTH, COLS), BF16),
                vmem((CHIPS * ROWS, COLS), F32),
                vmem((CHIPS, ROWS, COLS), BF16),
                vmem((KV, ROWS, COLS), BF16),
                vmem((ROWS * HEADS, D), F32),
                vmem((ROWS, D, SEQ * KV), BF16),
                vmem((HALF, WIDTH), BF16),
                vmem((ROWS + 1, MY, D), F32),
                vmem((ROWS + 1, MY, D), F32),
                vmem((3, ROWS * MY, D), F32),
                vmem((ROWS * MY, D), F32),
                vmem((ROWS * MY, D), F32),
                vmem((2, ROWS * 2 * KV, D), F32),
                vmem((ROWS * MY, D), F32),
                vmem((16, HALF), F32),
                vmem((ROWS, WIDTH), F32),
                vmem((ROWS, WIDTH), F32),
                dma((3,)), dma, dma((2,)), dma((len(OUT_PARTS),)),
                dma, dma((CHIPS - 1,)), dma, dma, dma, dma, dma, dma, dma, dma,
            ],
            compiler_params=pltpu.CompilerParams(
                collective_id=0, has_side_effects=True, vmem_limit_bytes=56 * 1024 * 1024),
            cost_estimate=pl.CostEstimate(flops=10 ** 9, bytes_accessed=6 * 10 ** 7, transcendentals=10 ** 6),
        )(hidden, w_query, w_key, w_value, w_out, k_cache.reshape(pairs), v_cache.reshape(pairs), write_pos)
        return pl.pallas_call(
            finish_kernel,
            out_shape=[jax.ShapeDtypeStruct(hidden.shape, BF16)] + [jax.ShapeDtypeStruct(shape, BF16)] * 2,
            in_specs=[any_spec] * 3,
            out_specs=[any_spec] * 3,
            scratch_shapes=[dma((3,))],
            compiler_params=pltpu.CompilerParams(vmem_limit_bytes=1024 * 1024),
            cost_estimate=pl.CostEstimate(flops=10 ** 6, bytes_accessed=10 ** 7, transcendentals=0),
        )(attn, k_old.reshape(shape), v_old.reshape(shape))

    return jax.shard_map(local_step, mesh=mesh, in_specs=(row_spec, P(), P(), P(), P('sp', None), cache_spec, cache_spec, len_spec, len_spec), out_specs=(row_spec, cache_spec, cache_spec), check_vma=False)
```

```python
import functools

import jax
import jax.numpy as jnp
from jax import lax
from jax.experimental import pallas as pl
from jax.experimental.pallas import tpu as pltpu
from jax.sharding import PartitionSpec as P

MESH = pl.DeviceIdType.MESH
BF16, F32 = jnp.bfloat16, jnp.float32

ROWS = 4
CHIPS = 4
D = 128
KV = 8
GROUP = 6
HEADS = KV * GROUP
WIDTH = 6144
HALF = WIDTH // 2
COLS = (GROUP + 2) * D
QCOLS = GROUP * D
SEQ = 256
MY = HEADS // 2
OUT_PARTS = [(0, 3072), (3072, 2048), (5120, 1024)]
NEG = -1e30
EXP2_SCALE = D ** -0.5 * 1.4426950408889634


def step_kernel(y_stride, hidden, w_query, w_key, w_value, w_out, k_cache, v_cache, write_pos,
                attn_out, kbuf, vbuf,
                pos_smem, gather, x32, w_in, proj, proj_send, proj_recv, q_rows, k_turned, w_o,
                part_send, part_recv, part_own, k_exp, v_exp, kv_rows, o_rows, o_lhs, out_send, out_recv,
                sem_misc, sem_w, sem_kv, sem_wo, send_a, recv_a, send_f, recv_f, send_b, recv_b,
                send_x, recv_x, send_p, recv_p):
    core = lax.axis_index('sp')
    other = 1 - core
    dp = lax.axis_index('dp')
    xb = lax.rem(dp, 2)
    yb = lax.rem(dp // y_stride, 2)
    dx, dy = 1 - 2 * xb, 1 - 2 * yb
    chip = [dp, dp + dx, dp + y_stride * dy, dp + dx + y_stride * dy]
    spot0 = xb + 2 * yb
    spot = [spot0, spot0 + dx, spot0 + 2 * dy, spot0 + dx + 2 * dy]
    cores = [core, other]
    mine = spot0 * 2 + core

    def dev(r, d):
        return {'dp': chip[r], 'sp': cores[d]}

    peers = [(3, 0), (3, 1), (1, 0), (1, 1), (2, 0), (2, 1), (0, 1)]

    col_q = pl.ds(pl.multiple_of(mine * QCOLS, D), QCOLS)
    col_k = pl.ds(pl.multiple_of(mine * D, D), D)
    q_load = pltpu.make_async_copy(w_query.at[:, col_q], w_in.at[:, pl.ds(0, QCOLS)], sem_w)
    kv_loads = [pltpu.make_async_copy(src.at[:, col_k], w_in.at[:, pl.ds(QCOLS + D * i, D)], sem_w)
                for i, src in enumerate((w_key, w_value))]

    def wo_copy(n):
        cols = pl.ds(OUT_PARTS[n][0], OUT_PARTS[n][1])
        return pltpu.make_async_copy(w_out.at[:, cols], w_o.at[:, cols], sem_wo.at[n])

    k_load = pltpu.make_async_copy(k_cache, kbuf, sem_kv.at[0])
    v_load = pltpu.make_async_copy(v_cache, vbuf, sem_kv.at[1])

    own = [pltpu.make_async_copy(hidden.at[:, pl.ds(h * HALF, HALF)], gather.at[0, h], sem_misc.at[h])
           for h in range(2)]
    pos_copy = pltpu.make_async_copy(write_pos, pos_smem, sem_misc.at[2])
    for cp in (*own, pos_copy, *kv_loads):
        cp.start()

    barrier = pltpu.get_barrier_semaphore()
    for r, d in peers:
        pl.semaphore_signal(barrier, inc=1, device_id=dev(r, d), device_id_type=MESH)
    for cp in own:
        cp.wait()
    q_load.start()
    for n in range(len(OUT_PARTS)):
        wo_copy(n).start(priority=1)
    for h in range(2):
        x32[h, 0:ROWS, :] = gather[0, h].astype(F32)
    pl.semaphore_wait(barrier, len(peers))

    def a_copy(r):
        return pltpu.make_async_remote_copy(gather.at[0, core], gather.at[r, core], send_a, recv_a.at[r - 1],
                                            device_id=dev(r, 0), device_id_type=MESH)

    def f_copy(r):
        return pltpu.make_async_remote_copy(gather.at[r, core], gather.at[r, core], send_f, recv_f,
                                            device_id=dev(0, 1), device_id_type=MESH)

    def whole(ref, send, recv):
        return pltpu.make_async_remote_copy(ref, ref, send, recv, device_id=dev(0, 1), device_id_type=MESH)

    for r in (3, 1, 2):
        a_copy(r).start()


    for r in (1, 2, 3):
        a_copy(r).wait_recv()
        f_copy(r).start()
        if r == 1:
            for cp in (k_load, v_load):
                cp.start()
        x32[core, ROWS * r:ROWS * (r + 1), :] = gather[r, core].astype(F32)

    def project(half):
        rows = pl.ds(pl.multiple_of(half * HALF, HALF), HALF)
        return jnp.dot(x32[half].astype(BF16), w_in[rows, :], preferred_element_type=F32)

    pltpu.make_async_copy(w_in, w_in, sem_w).wait()
    proj[...] = project(core)
    whole(gather.at[1:CHIPS, other], send_f, recv_f).wait_recv()
    for r in (1, 2, 3):
        x32[other, ROWS * r:ROWS * (r + 1), :] = gather[r, other].astype(F32)
    proj[...] += project(other)

    def b_copy(r, d):
        return pltpu.make_async_remote_copy(proj_send.at[r], proj_recv.at[mine], send_b, recv_b,
                                            device_id=dev(r, d), device_id_type=MESH)

    for r in (3, 1, 2, 0):
        proj_send[r] = proj[ROWS * r:ROWS * (r + 1), :].astype(BF16)
        for d in range(0 if r else 1, 2):
            b_copy(r, d).start()
    proj_recv[mine] = proj_send[0]
    k_load.wait()
    for b in range(ROWS):
        k_turned[b] = kbuf[b].reshape(SEQ * KV, D).T
    pos_copy.wait()
    whole(proj_recv.at[0:len(peers)], send_b, recv_b).wait_recv()

    for e in range(KV):
        block = proj_recv[e].astype(F32)
        for j in range(GROUP):
            q_rows[pl.ds(GROUP * e + j, ROWS, stride=HEADS), :] = block[:, D * j:D * (j + 1)]

    v_load.wait()
    lane = lax.broadcasted_iota(jnp.int32, (HEADS, D), 1)
    head = lax.broadcasted_iota(jnp.int32, (HEADS, D), 0)
    same_kv = lax.rem(lane, KV) == head // GROUP
    step = lane // KV
    stat_of = lane // (D // (2 * ROWS))
    blocks = SEQ * KV // D
    per_block = D // KV

    def scores(b):
        q = q_rows[HEADS * b:HEADS * (b + 1), :].astype(BF16)
        return jnp.dot(q, k_turned[b], preferred_element_type=F32)

    def soften(b, s):
        limit = pos_smem[b] - core * SEQ
        tiles = [jnp.where(same_kv & (step < limit - per_block * j), s[:, D * j:D * (j + 1)], NEG)
                 for j in range(blocks)]
        top = functools.reduce(jnp.maximum, tiles)
        top = jnp.max(top, axis=1, keepdims=True)
        tiles = [jnp.exp2((t - top) * EXP2_SCALE) for t in tiles]
        total = jnp.sum(functools.reduce(jnp.add, tiles), axis=1, keepdims=True)
        return top, total, jnp.concatenate([t.astype(BF16) for t in tiles], axis=1)

    def values(b, top, total, p):
        acc = jnp.dot(p, vbuf[b].reshape(SEQ * KV, D), preferred_element_type=F32)
        rows = slice(MY * b, MY * (b + 1))
        stats = jnp.where(stat_of == 2 * b, top, jnp.where(stat_of == 2 * b + 1, total, 0.0))
        part_send[b] = jnp.where(core == 0, acc[MY:HEADS], acc[0:MY])
        part_own[0, rows, :] = jnp.where(core == 0, acc[0:MY], acc[MY:HEADS])
        for i, v in enumerate((top, total)):
            part_own[1 + i, rows, :] = jnp.broadcast_to(jnp.where(core == 0, v[0:MY], v[MY:HEADS]), (MY, D))
        return stats

    raw = [scores(b) for b in range(ROWS)]
    soft = [soften(b, raw[b]) for b in range(ROWS)]
    stats = functools.reduce(jnp.add, [values(b, *soft[b]) for b in range(ROWS)])
    part_send[ROWS] = jnp.where(core == 0, stats[MY:HEADS], stats[0:MY])
    x_copy = pltpu.make_async_remote_copy(part_send, part_recv, send_x, recv_x,
                                          device_id=dev(0, 1), device_id_type=MESH)
    x_copy.start()

    for i in range(KV // 2):
        block = proj_recv[core * (KV // 2) + i].astype(F32)
        for j in range(GROUP):
            at = pl.ds(GROUP * i + j, ROWS, stride=MY)
            k_exp[at, :] = block[:, QCOLS:QCOLS + D]
            v_exp[at, :] = block[:, QCOLS + D:]
    for e in range(KV):
        block = proj_recv[e].astype(F32)
        for i in range(2):
            for at in (e, e + KV):
                kv_rows[i, pl.ds(at, ROWS, stride=2 * KV), :] = block[:, QCOLS + D * i:QCOLS + D * (i + 1)]
    q_mine = jnp.concatenate([q_rows[pl.ds(pl.multiple_of(HEADS * b + MY * core, 8), MY), :] for b in range(ROWS)], axis=0)
    s_new = jnp.sum(q_mine * k_exp[...], axis=1, keepdims=True)

    tick = (lax.broadcasted_iota(jnp.int32, (16, 16, D), 0) * 2
            + lax.broadcasted_iota(jnp.int32, (16, 16, D), 1) // KV).astype(F32).astype(BF16)

    def put(which, buf):
        def body(i, _):
            rows = pl.ds(pl.multiple_of(i * 16, 16), 16)
            for b in range(ROWS):
                want = (pos_smem[b] - core * SEQ - i * 32).astype(F32).astype(BF16)
                new = kv_rows[which, 2 * KV * b:2 * KV * (b + 1), :].astype(BF16)
                buf[b, rows] = jnp.where(tick == want, new[None], buf[b, rows])
            return 0
        lax.fori_loop(0, SEQ // 32, body, 0)

    put(0, kbuf)

    x_copy.wait_recv()
    stats = part_recv[ROWS]
    peer = [part_recv[0:ROWS].reshape(ROWS * MY, D)]
    for i in range(2):
        lanes = [D // (2 * ROWS) * (2 * b + i) for b in range(ROWS)]
        peer.append(jnp.concatenate([jnp.broadcast_to(stats[:, at:at + 1], (MY, D)) for at in lanes], axis=0))
    top = jnp.maximum(jnp.maximum(part_own[1], peer[1]), s_new)
    w_own = jnp.exp2((part_own[1] - top) * EXP2_SCALE)
    w_peer = jnp.exp2((peer[1] - top) * EXP2_SCALE)
    w_new = jnp.exp2((s_new - top) * EXP2_SCALE)
    total = part_own[2] * w_own + peer[2] * w_peer + w_new
    o_rows[...] = (part_own[0] * w_own + peer[0] * w_peer + v_exp[...] * w_new) / total

    o_lhs[...] = jnp.zeros_like(o_lhs)
    for h in range(MY):
        o_lhs[0:ROWS, D * h:D * (h + 1)] = o_rows[pl.ds(h, ROWS, stride=MY), :]
    o_bf = o_lhs[...].astype(BF16)

    def p_copy(n):
        cols = pl.ds(OUT_PARTS[n][0], OUT_PARTS[n][1])
        return pltpu.make_async_remote_copy(out_send.at[:, cols], out_recv.at[:, cols], send_p, recv_p,
                                            device_id=dev(0, 1), device_id_type=MESH)

    for n, (at, width) in enumerate(OUT_PARTS):
        wo_copy(n).wait()
        out_send[:, at:at + width] = jnp.dot(o_bf, w_o[:, at:at + width], preferred_element_type=F32)[0:ROWS]
        p_copy(n).start()
    put(1, vbuf)
    whole(out_recv, send_p, recv_p).wait_recv()
    attn_out[...] = (out_send[...] + out_recv[...]).astype(BF16)

    whole(gather.at[1:CHIPS, core], send_a, recv_a.at[0]).wait_send()
    whole(gather.at[1:CHIPS, core], send_f, recv_f).wait_send()
    whole(proj_recv.at[0:len(peers)], send_b, recv_b).wait_send()
    x_copy.wait_send()
    whole(out_send, send_p, recv_p).wait_send()


def finish_kernel(attn, k_old, v_old, attn_out, k_next, v_next, sem):
    copies = [pltpu.make_async_copy(src, dst, sem.at[i])
              for i, (src, dst) in enumerate(((k_old, k_next), (v_old, v_next), (attn, attn_out)))]
    for cp in copies:
        cp.start()
    for cp in copies:
        cp.wait()


def solution(mesh):
    row_spec = P(('rep', 'dp'), None)
    cache_spec = P(('rep', 'dp'), 'sp', None, None)
    len_spec = P(('rep', 'dp'))
    y_stride = 4 if mesh.shape['dp'] >= 8 else 2

    def local_step(hidden, w_query, w_key, w_value, w_out, k_cache, v_cache, write_pos, valid_len):
        shape = k_cache.shape
        pairs = (ROWS, SEQ * KV // 16, 16, D)
        any_spec = pl.BlockSpec(memory_space=pl.ANY)
        vmem = pltpu.VMEM
        dma = pltpu.SemaphoreType.DMA
        attn, k_old, v_old = pl.pallas_call(
            functools.partial(step_kernel, y_stride),
            out_shape=[vmem(hidden.shape, BF16), vmem(pairs, BF16), vmem(pairs, BF16)],
            in_specs=[any_spec] * 8,
            out_specs=[pl.BlockSpec(memory_space=vmem)] * 3,
            scratch_shapes=[
                pltpu.SMEM((ROWS,), jnp.int32),
                vmem((CHIPS, 2, ROWS, HALF), BF16),
                vmem((2, CHIPS * ROWS, HALF), F32),
                vmem((WIDTH, COLS), BF16),
                vmem((CHIPS * ROWS, COLS), F32),
                vmem((CHIPS, ROWS, COLS), BF16),
                vmem((KV, ROWS, COLS), BF16),
                vmem((ROWS * HEADS, D), F32),
                vmem((ROWS, D, SEQ * KV), BF16),
                vmem((HALF, WIDTH), BF16),
                vmem((ROWS + 1, MY, D), F32),
                vmem((ROWS + 1, MY, D), F32),
                vmem((3, ROWS * MY, D), F32),
                vmem((ROWS * MY, D), F32),
                vmem((ROWS * MY, D), F32),
                vmem((2, ROWS * 2 * KV, D), F32),
                vmem((ROWS * MY, D), F32),
                vmem((16, HALF), F32),
                vmem((ROWS, WIDTH), F32),
                vmem((ROWS, WIDTH), F32),
                dma((3,)), dma, dma((2,)), dma((len(OUT_PARTS),)),
                dma, dma((CHIPS - 1,)), dma, dma, dma, dma, dma, dma, dma, dma,
            ],
            compiler_params=pltpu.CompilerParams(
                collective_id=0, has_side_effects=True, vmem_limit_bytes=56 * 1024 * 1024),
            cost_estimate=pl.CostEstimate(flops=10 ** 9, bytes_accessed=6 * 10 ** 7, transcendentals=10 ** 6),
        )(hidden, w_query, w_key, w_value, w_out, k_cache.reshape(pairs), v_cache.reshape(pairs), write_pos)
        return pl.pallas_call(
            finish_kernel,
            out_shape=[jax.ShapeDtypeStruct(hidden.shape, BF16)] + [jax.ShapeDtypeStruct(shape, BF16)] * 2,
            in_specs=[any_spec] * 3,
            out_specs=[any_spec] * 3,
            scratch_shapes=[dma((3,))],
            compiler_params=pltpu.CompilerParams(vmem_limit_bytes=1024 * 1024),
            cost_estimate=pl.CostEstimate(flops=10 ** 6, bytes_accessed=10 ** 7, transcendentals=0),
        )(attn, k_old.reshape(shape), v_old.reshape(shape))

    return jax.shard_map(local_step, mesh=mesh, in_specs=(row_spec, P(), P(), P(), P('sp', None), cache_spec, cache_spec, len_spec, len_spec), out_specs=(row_spec, cache_spec, cache_spec), check_vma=False)
```

```python
import functools

import jax
import jax.numpy as jnp
from jax import lax
from jax.experimental import pallas as pl
from jax.experimental.pallas import tpu as pltpu
from jax.sharding import PartitionSpec as P

MESH = pl.DeviceIdType.MESH
BF16, F32 = jnp.bfloat16, jnp.float32

ROWS = 4
CHIPS = 4
D = 128
KV = 8
GROUP = 6
HEADS = KV * GROUP
WIDTH = 6144
HALF = WIDTH // 2
COLS = (GROUP + 2) * D
QCOLS = GROUP * D
SEQ = 256
MY = HEADS // 2
OUT_PARTS = [(0, 4096), (4096, 2048)]
NEG = -3e38
EXP2_SCALE = D ** -0.5 * 1.4426950408889634


def step_kernel(y_stride, hidden, w_query, w_key, w_value, w_out, k_cache, v_cache, write_pos,
                attn_out, kbuf, vbuf,
                pos_smem, gather, x32, w_in, proj, proj_send, proj_recv, q_rows, k_turned, w_o,
                part_send, part_recv, part_own, k_exp, v_exp, kv_rows, o_rows, o_lhs, out_send, out_recv,
                sem_misc, sem_w, sem_kv, sem_wo, send_a, recv_a, send_f, recv_f, send_b, recv_b,
                send_x, recv_x, send_p, recv_p):
    core = lax.axis_index('sp')
    other = 1 - core
    dp = lax.axis_index('dp')
    xb = lax.rem(dp, 2)
    yb = lax.rem(dp // y_stride, 2)
    dx, dy = 1 - 2 * xb, 1 - 2 * yb
    chip = [dp, dp + dx, dp + y_stride * dy, dp + dx + y_stride * dy]
    spot0 = xb + 2 * yb
    spot = [spot0, spot0 + dx, spot0 + 2 * dy, spot0 + dx + 2 * dy]
    cores = [core, other]
    mine = spot0 * 2 + core

    def dev(r, d):
        return {'dp': chip[r], 'sp': cores[d]}

    peers = [(3, 0), (3, 1), (1, 0), (1, 1), (2, 0), (2, 1), (0, 1)]

    col_q = pl.ds(pl.multiple_of(mine * QCOLS, D), QCOLS)
    col_k = pl.ds(pl.multiple_of(mine * D, D), D)
    q_load = pltpu.make_async_copy(w_query.at[:, col_q], w_in.at[:, pl.ds(0, QCOLS)], sem_w)
    kv_loads = [pltpu.make_async_copy(src.at[:, col_k], w_in.at[:, pl.ds(QCOLS + D * i, D)], sem_w)
                for i, src in enumerate((w_key, w_value))]

    def wo_copy(n):
        cols = pl.ds(OUT_PARTS[n][0], OUT_PARTS[n][1])
        return pltpu.make_async_copy(w_out.at[:, cols], w_o.at[:, cols], sem_wo.at[n])

    k_load = pltpu.make_async_copy(k_cache, kbuf, sem_kv.at[0])
    v_load = pltpu.make_async_copy(v_cache, vbuf, sem_kv.at[1])

    own = [pltpu.make_async_copy(hidden.at[:, pl.ds(h * HALF, HALF)], gather.at[0, h], sem_misc.at[h])
           for h in range(2)]
    pos_copy = pltpu.make_async_copy(write_pos, pos_smem, sem_misc.at[2])
    for cp in (*own, pos_copy, *kv_loads):
        cp.start()

    barrier = pltpu.get_barrier_semaphore()
    for r, d in peers:
        pl.semaphore_signal(barrier, inc=1, device_id=dev(r, d), device_id_type=MESH)
    for cp in own:
        cp.wait()
    q_load.start()
    for n in range(len(OUT_PARTS)):
        wo_copy(n).start(priority=1)
    for h in range(2):
        x32[h, 0:ROWS, :] = gather[0, h].astype(F32)
    pl.semaphore_wait(barrier, len(peers))

    def a_copy(r):
        return pltpu.make_async_remote_copy(gather.at[0, core], gather.at[r, core], send_a, recv_a.at[r - 1],
                                            device_id=dev(r, 0), device_id_type=MESH)

    def f_copy(r):
        return pltpu.make_async_remote_copy(gather.at[r, core], gather.at[r, core], send_f, recv_f,
                                            device_id=dev(0, 1), device_id_type=MESH)

    def whole(ref, send, recv):
        return pltpu.make_async_remote_copy(ref, ref, send, recv, device_id=dev(0, 1), device_id_type=MESH)

    for r in (3, 1, 2):
        a_copy(r).start()


    for r in (1, 2, 3):
        a_copy(r).wait_recv()
        f_copy(r).start()
        if r == 1:
            for cp in (k_load, v_load):
                cp.start()
        x32[core, ROWS * r:ROWS * (r + 1), :] = gather[r, core].astype(F32)

    def project(half):
        rows = pl.ds(pl.multiple_of(half * HALF, HALF), HALF)
        return jnp.dot(x32[half].astype(BF16), w_in[rows, :], preferred_element_type=F32)

    pltpu.make_async_copy(w_in, w_in, sem_w).wait()
    proj[...] = project(core)
    whole(gather.at[1:CHIPS, other], send_f, recv_f).wait_recv()
    for r in (1, 2, 3):
        x32[other, ROWS * r:ROWS * (r + 1), :] = gather[r, other].astype(F32)
    proj[...] += project(other)

    def b_copy(r, d):
        return pltpu.make_async_remote_copy(proj_send.at[r], proj_recv.at[mine], send_b, recv_b,
                                            device_id=dev(r, d), device_id_type=MESH)

    for r in (3, 1, 2, 0):
        proj_send[r] = proj[ROWS * r:ROWS * (r + 1), :].astype(BF16)
        for d in range(0 if r else 1, 2):
            b_copy(r, d).start()
    proj_recv[mine] = proj_send[0]
    k_load.wait()
    for b in range(ROWS):
        k_turned[b] = kbuf[b].reshape(SEQ * KV, D).T
    pos_copy.wait()
    whole(proj_recv.at[0:len(peers)], send_b, recv_b).wait_recv()

    for e in range(KV):
        block = proj_recv[e].astype(F32)
        for j in range(GROUP):
            q_rows[pl.ds(GROUP * e + j, ROWS, stride=HEADS), :] = block[:, D * j:D * (j + 1)]

    v_load.wait()
    lane = lax.broadcasted_iota(jnp.int32, (HEADS, D), 1)
    head = lax.broadcasted_iota(jnp.int32, (HEADS, D), 0)
    same_kv = lax.rem(lane, KV) == head // GROUP
    step = lane // KV
    stat_of = lane // (D // (2 * ROWS))
    blocks = SEQ * KV // D
    per_block = D // KV

    def scores(b):
        q = q_rows[HEADS * b:HEADS * (b + 1), :].astype(BF16)
        return jnp.dot(q, k_turned[b], preferred_element_type=F32)

    def soften(b, s):
        limit = pos_smem[b] - core * SEQ
        tiles = [jnp.where(same_kv & (step < limit - per_block * j), s[:, D * j:D * (j + 1)], NEG)
                 for j in range(blocks)]
        top = functools.reduce(jnp.maximum, tiles)
        top = jnp.max(top, axis=1, keepdims=True)
        tiles = [jnp.exp2((t - top) * EXP2_SCALE) for t in tiles]
        total = jnp.sum(functools.reduce(jnp.add, tiles), axis=1, keepdims=True)
        return top, total, jnp.concatenate([t.astype(BF16) for t in tiles], axis=1)

    def values(b, top, total, p):
        acc = jnp.dot(p, vbuf[b].reshape(SEQ * KV, D), preferred_element_type=F32)
        rows = slice(MY * b, MY * (b + 1))
        stats = jnp.where(stat_of == 2 * b, top, jnp.where(stat_of == 2 * b + 1, total, 0.0))
        part_send[b] = jnp.where(core == 0, acc[MY:HEADS], acc[0:MY])
        part_own[0, rows, :] = jnp.where(core == 0, acc[0:MY], acc[MY:HEADS])
        for i, v in enumerate((top, total)):
            part_own[1 + i, rows, :] = jnp.broadcast_to(jnp.where(core == 0, v[0:MY], v[MY:HEADS]), (MY, D))
        return stats

    raw = [scores(b) for b in range(ROWS)]
    soft = [soften(b, raw[b]) for b in range(ROWS)]
    stats = functools.reduce(jnp.add, [values(b, *soft[b]) for b in range(ROWS)])
    part_send[ROWS] = jnp.where(core == 0, stats[MY:HEADS], stats[0:MY])
    x_copy = pltpu.make_async_remote_copy(part_send, part_recv, send_x, recv_x,
                                          device_id=dev(0, 1), device_id_type=MESH)
    x_copy.start()

    for i in range(KV // 2):
        block = proj_recv[core * (KV // 2) + i].astype(F32)
        for j in range(GROUP):
            at = pl.ds(GROUP * i + j, ROWS, stride=MY)
            k_exp[at, :] = block[:, QCOLS:QCOLS + D]
            v_exp[at, :] = block[:, QCOLS + D:]
    for e in range(KV):
        block = proj_recv[e].astype(F32)
        for i in range(2):
            for at in (e, e + KV):
                kv_rows[i, pl.ds(at, ROWS, stride=2 * KV), :] = block[:, QCOLS + D * i:QCOLS + D * (i + 1)]
    q_mine = jnp.concatenate([q_rows[pl.ds(pl.multiple_of(HEADS * b + MY * core, 8), MY), :] for b in range(ROWS)], axis=0)
    s_new = jnp.sum(q_mine * k_exp[...], axis=1, keepdims=True)

    tick = (lax.broadcasted_iota(jnp.int32, (16, 16, D), 0) * 2
            + lax.broadcasted_iota(jnp.int32, (16, 16, D), 1) // KV).astype(F32).astype(BF16)

    def put(which, buf):
        def body(i, _):
            rows = pl.ds(pl.multiple_of(i * 16, 16), 16)
            for b in range(ROWS):
                want = (pos_smem[b] - core * SEQ - i * 32).astype(F32).astype(BF16)
                new = kv_rows[which, 2 * KV * b:2 * KV * (b + 1), :].astype(BF16)
                buf[b, rows] = jnp.where(tick == want, new[None], buf[b, rows])
            return 0
        lax.fori_loop(0, SEQ // 32, body, 0)

    put(0, kbuf)

    x_copy.wait_recv()
    stats = part_recv[ROWS]
    peer = [part_recv[0:ROWS].reshape(ROWS * MY, D)]
    for i in range(2):
        lanes = [D // (2 * ROWS) * (2 * b + i) for b in range(ROWS)]
        peer.append(jnp.concatenate([jnp.broadcast_to(stats[:, at:at + 1], (MY, D)) for at in lanes], axis=0))
    top = jnp.maximum(jnp.maximum(part_own[1], peer[1]), s_new)
    w_own = jnp.exp2((part_own[1] - top) * EXP2_SCALE)
    w_peer = jnp.exp2((peer[1] - top) * EXP2_SCALE)
    w_new = jnp.exp2((s_new - top) * EXP2_SCALE)
    total = part_own[2] * w_own + peer[2] * w_peer + w_new
    o_rows[...] = (part_own[0] * w_own + peer[0] * w_peer + v_exp[...] * w_new) / total

    o_lhs[...] = jnp.zeros_like(o_lhs)
    for h in range(MY):
        o_lhs[0:ROWS, D * h:D * (h + 1)] = o_rows[pl.ds(h, ROWS, stride=MY), :]
    o_bf = o_lhs[...].astype(BF16)

    def p_copy(n):
        cols = pl.ds(OUT_PARTS[n][0], OUT_PARTS[n][1])
        return pltpu.make_async_remote_copy(out_send.at[:, cols], out_recv.at[:, cols], send_p, recv_p,
                                            device_id=dev(0, 1), device_id_type=MESH)

    for n, (at, width) in enumerate(OUT_PARTS):
        wo_copy(n).wait()
        out_send[:, at:at + width] = jnp.dot(o_bf, w_o[:, at:at + width], preferred_element_type=F32)[0:ROWS]
        p_copy(n).start()
    put(1, vbuf)
    whole(out_recv, send_p, recv_p).wait_recv()
    attn_out[...] = (out_send[...] + out_recv[...]).astype(BF16)

    whole(gather.at[1:CHIPS, core], send_a, recv_a.at[0]).wait_send()
    whole(gather.at[1:CHIPS, core], send_f, recv_f).wait_send()
    whole(proj_recv.at[0:len(peers)], send_b, recv_b).wait_send()
    x_copy.wait_send()
    whole(out_send, send_p, recv_p).wait_send()


def finish_kernel(attn, k_old, v_old, attn_out, k_next, v_next, sem):
    copies = [pltpu.make_async_copy(src, dst, sem.at[i])
              for i, (src, dst) in enumerate(((k_old, k_next), (v_old, v_next), (attn, attn_out)))]
    for cp in copies:
        cp.start()
    for cp in copies:
        cp.wait()


def solution(mesh):
    row_spec = P(('rep', 'dp'), None)
    cache_spec = P(('rep', 'dp'), 'sp', None, None)
    len_spec = P(('rep', 'dp'))
    y_stride = 4 if mesh.shape['dp'] >= 8 else 2

    def local_step(hidden, w_query, w_key, w_value, w_out, k_cache, v_cache, write_pos, valid_len):
        shape = k_cache.shape
        pairs = (ROWS, SEQ * KV // 16, 16, D)
        any_spec = pl.BlockSpec(memory_space=pl.ANY)
        vmem = pltpu.VMEM
        dma = pltpu.SemaphoreType.DMA
        attn, k_old, v_old = pl.pallas_call(
            functools.partial(step_kernel, y_stride),
            out_shape=[vmem(hidden.shape, BF16), vmem(pairs, BF16), vmem(pairs, BF16)],
            in_specs=[any_spec] * 8,
            out_specs=[pl.BlockSpec(memory_space=vmem)] * 3,
            scratch_shapes=[
                pltpu.SMEM((ROWS,), jnp.int32),
                vmem((CHIPS, 2, ROWS, HALF), BF16),
                vmem((2, CHIPS * ROWS, HALF), F32),
                vmem((WIDTH, COLS), BF16),
                vmem((CHIPS * ROWS, COLS), F32),
                vmem((CHIPS, ROWS, COLS), BF16),
                vmem((KV, ROWS, COLS), BF16),
                vmem((ROWS * HEADS, D), F32),
                vmem((ROWS, D, SEQ * KV), BF16),
                vmem((HALF, WIDTH), BF16),
                vmem((ROWS + 1, MY, D), F32),
                vmem((ROWS + 1, MY, D), F32),
                vmem((3, ROWS * MY, D), F32),
                vmem((ROWS * MY, D), F32),
                vmem((ROWS * MY, D), F32),
                vmem((2, ROWS * 2 * KV, D), F32),
                vmem((ROWS * MY, D), F32),
                vmem((16, HALF), F32),
                vmem((ROWS, WIDTH), F32),
                vmem((ROWS, WIDTH), F32),
                dma((3,)), dma, dma((2,)), dma((len(OUT_PARTS),)),
                dma, dma((CHIPS - 1,)), dma, dma, dma, dma, dma, dma, dma, dma,
            ],
            compiler_params=pltpu.CompilerParams(
                collective_id=0, has_side_effects=True, vmem_limit_bytes=56 * 1024 * 1024),
            cost_estimate=pl.CostEstimate(flops=10 ** 9, bytes_accessed=6 * 10 ** 7, transcendentals=10 ** 6),
        )(hidden, w_query, w_key, w_value, w_out, k_cache.reshape(pairs), v_cache.reshape(pairs), write_pos)
        return pl.pallas_call(
            finish_kernel,
            out_shape=[jax.ShapeDtypeStruct(hidden.shape, BF16)] + [jax.ShapeDtypeStruct(shape, BF16)] * 2,
            in_specs=[any_spec] * 3,
            out_specs=[any_spec] * 3,
            scratch_shapes=[dma((3,))],
            compiler_params=pltpu.CompilerParams(vmem_limit_bytes=1024 * 1024),
            cost_estimate=pl.CostEstimate(flops=10 ** 6, bytes_accessed=10 ** 7, transcendentals=0),
        )(attn, k_old.reshape(shape), v_old.reshape(shape))

    return jax.shard_map(local_step, mesh=mesh, in_specs=(row_spec, P(), P(), P(), P('sp', None), cache_spec, cache_spec, len_spec, len_spec), out_specs=(row_spec, cache_spec, cache_spec), check_vma=False)
```

```python
import functools

import jax
import jax.numpy as jnp
from jax import lax
from jax.experimental import pallas as pl
from jax.experimental.pallas import tpu as pltpu
from jax.sharding import PartitionSpec as P

MESH = pl.DeviceIdType.MESH
BF16, F32 = jnp.bfloat16, jnp.float32

ROWS = 4
CHIPS = 4
D = 128
KV = 8
GROUP = 6
HEADS = KV * GROUP
WIDTH = 6144
HALF = WIDTH // 2
COLS = (GROUP + 2) * D
QCOLS = GROUP * D
SEQ = 256
MY = HEADS // 2
OUT_PARTS = [(0, 3072), (3072, 2048), (5120, 1024)]
NEG = -3e38
EXP2_SCALE = D ** -0.5 * 1.4426950408889634


def step_kernel(y_stride, hidden, w_query, w_key, w_value, w_out, k_cache, v_cache, write_pos,
                attn_out, kbuf, vbuf,
                pos_smem, gather, x32, w_in, proj, proj_send, proj_recv, q_rows, k_turned, w_o,
                part_send, part_recv, part_own, k_exp, v_exp, kv_rows, o_rows, o_lhs, out_send, out_recv,
                sem_misc, sem_w, sem_kv, sem_wo, send_a, recv_a, send_f, recv_f, send_b, recv_b,
                send_x, recv_x, send_p, recv_p):
    core = lax.axis_index('sp')
    other = 1 - core
    dp = lax.axis_index('dp')
    xb = lax.rem(dp, 2)
    yb = lax.rem(dp // y_stride, 2)
    dx, dy = 1 - 2 * xb, 1 - 2 * yb
    chip = [dp, dp + dx, dp + y_stride * dy, dp + dx + y_stride * dy]
    spot0 = xb + 2 * yb
    spot = [spot0, spot0 + dx, spot0 + 2 * dy, spot0 + dx + 2 * dy]
    cores = [core, other]
    mine = spot0 * 2 + core

    def dev(r, d):
        return {'dp': chip[r], 'sp': cores[d]}

    peers = [(3, 0), (3, 1), (1, 0), (1, 1), (2, 0), (2, 1), (0, 1)]

    col_q = pl.ds(pl.multiple_of(mine * QCOLS, D), QCOLS)
    col_k = pl.ds(pl.multiple_of(mine * D, D), D)
    q_load = pltpu.make_async_copy(w_query.at[:, col_q], w_in.at[:, pl.ds(0, QCOLS)], sem_w)
    kv_loads = [pltpu.make_async_copy(src.at[:, col_k], w_in.at[:, pl.ds(QCOLS + D * i, D)], sem_w)
                for i, src in enumerate((w_key, w_value))]

    def wo_copy(n):
        cols = pl.ds(OUT_PARTS[n][0], OUT_PARTS[n][1])
        return pltpu.make_async_copy(w_out.at[:, cols], w_o.at[:, cols], sem_wo.at[n])

    k_load = pltpu.make_async_copy(k_cache, kbuf, sem_kv.at[0])
    v_load = pltpu.make_async_copy(v_cache, vbuf, sem_kv.at[1])

    own = [pltpu.make_async_copy(hidden.at[:, pl.ds(h * HALF, HALF)], gather.at[0, h], sem_misc.at[h])
           for h in range(2)]
    pos_copy = pltpu.make_async_copy(write_pos, pos_smem, sem_misc.at[2])
    for cp in (*own, pos_copy, *kv_loads):
        cp.start()

    barrier = pltpu.get_barrier_semaphore()
    for r, d in peers:
        pl.semaphore_signal(barrier, inc=1, device_id=dev(r, d), device_id_type=MESH)
    for cp in own:
        cp.wait()
    q_load.start()
    for n in range(len(OUT_PARTS)):
        wo_copy(n).start(priority=1)
    for h in range(2):
        x32[h, 0:ROWS, :] = gather[0, h].astype(F32)
    pl.semaphore_wait(barrier, len(peers))

    def a_copy(r):
        return pltpu.make_async_remote_copy(gather.at[0, core], gather.at[r, core], send_a, recv_a.at[r - 1],
                                            device_id=dev(r, 0), device_id_type=MESH)

    def f_copy(r):
        return pltpu.make_async_remote_copy(gather.at[r, core], gather.at[r, core], send_f, recv_f,
                                            device_id=dev(0, 1), device_id_type=MESH)

    def whole(ref, send, recv):
        return pltpu.make_async_remote_copy(ref, ref, send, recv, device_id=dev(0, 1), device_id_type=MESH)

    for r in (3, 1, 2):
        a_copy(r).start()


    for r in (1, 2, 3):
        a_copy(r).wait_recv()
        f_copy(r).start()
        if r == 1:
            for cp in (k_load, v_load):
                cp.start()
        x32[core, ROWS * r:ROWS * (r + 1), :] = gather[r, core].astype(F32)

    def project(half):
        rows = pl.ds(pl.multiple_of(half * HALF, HALF), HALF)
        return jnp.dot(x32[half].astype(BF16), w_in[rows, :], preferred_element_type=F32)

    pltpu.make_async_copy(w_in, w_in, sem_w).wait()
    proj[...] = project(core)
    whole(gather.at[1:CHIPS, other], send_f, recv_f).wait_recv()
    for r in (1, 2, 3):
        x32[other, ROWS * r:ROWS * (r + 1), :] = gather[r, other].astype(F32)
    proj[...] += project(other)

    def b_copy(r, d):
        return pltpu.make_async_remote_copy(proj_send.at[r], proj_recv.at[mine], send_b, recv_b,
                                            device_id=dev(r, d), device_id_type=MESH)

    for r in (3, 1, 2, 0):
        proj_send[r] = proj[ROWS * r:ROWS * (r + 1), :].astype(BF16)
        for d in range(0 if r else 1, 2):
            b_copy(r, d).start()
    proj_recv[mine] = proj_send[0]
    k_load.wait()
    for b in range(ROWS):
        k_turned[b] = kbuf[b].reshape(SEQ * KV, D).T
    pos_copy.wait()
    whole(proj_recv.at[0:len(peers)], send_b, recv_b).wait_recv()

    for e in range(KV):
        block = proj_recv[e].astype(F32)
        for j in range(GROUP):
            q_rows[pl.ds(GROUP * e + j, ROWS, stride=HEADS), :] = block[:, D * j:D * (j + 1)]

    v_load.wait()
    lane = lax.broadcasted_iota(jnp.int32, (HEADS, D), 1)
    head = lax.broadcasted_iota(jnp.int32, (HEADS, D), 0)
    same_kv = lax.rem(lane, KV) == head // GROUP
    step = lane // KV
    stat_of = lane // (D // (2 * ROWS))
    blocks = SEQ * KV // D
    per_block = D // KV

    def scores(b):
        q = q_rows[HEADS * b:HEADS * (b + 1), :].astype(BF16)
        return jnp.dot(q, k_turned[b], preferred_element_type=F32)

    def soften(b, s):
        limit = pos_smem[b] - core * SEQ
        tiles = [jnp.where(same_kv & (step < limit - per_block * j), s[:, D * j:D * (j + 1)], NEG)
                 for j in range(blocks)]
        top = functools.reduce(jnp.maximum, tiles)
        top = jnp.max(top, axis=1, keepdims=True)
        tiles = [jnp.exp2((t - top) * EXP2_SCALE) for t in tiles]
        total = jnp.sum(functools.reduce(jnp.add, tiles), axis=1, keepdims=True)
        return top, total, jnp.concatenate([t.astype(BF16) for t in tiles], axis=1)

    def values(b, top, total, p):
        acc = jnp.dot(p, vbuf[b].reshape(SEQ * KV, D), preferred_element_type=F32)
        rows = slice(MY * b, MY * (b + 1))
        stats = jnp.where(stat_of == 2 * b, top, jnp.where(stat_of == 2 * b + 1, total, 0.0))
        part_send[b] = jnp.where(core == 0, acc[MY:HEADS], acc[0:MY])
        part_own[0, rows, :] = jnp.where(core == 0, acc[0:MY], acc[MY:HEADS])
        for i, v in enumerate((top, total)):
            part_own[1 + i, rows, :] = jnp.broadcast_to(jnp.where(core == 0, v[0:MY], v[MY:HEADS]), (MY, D))
        return stats

    raw = [scores(b) for b in range(ROWS)]
    soft = [soften(b, raw[b]) for b in range(ROWS)]
    stats = functools.reduce(jnp.add, [values(b, *soft[b]) for b in range(ROWS)])
    part_send[ROWS] = jnp.where(core == 0, stats[MY:HEADS], stats[0:MY])
    x_copy = pltpu.make_async_remote_copy(part_send, part_recv, send_x, recv_x,
                                          device_id=dev(0, 1), device_id_type=MESH)
    x_copy.start()

    for i in range(KV // 2):
        block = proj_recv[core * (KV // 2) + i].astype(F32)
        for j in range(GROUP):
            at = pl.ds(GROUP * i + j, ROWS, stride=MY)
            k_exp[at, :] = block[:, QCOLS:QCOLS + D]
            v_exp[at, :] = block[:, QCOLS + D:]
    for e in range(KV):
        block = proj_recv[e].astype(F32)
        for i in range(2):
            for at in (e, e + KV):
                kv_rows[i, pl.ds(at, ROWS, stride=2 * KV), :] = block[:, QCOLS + D * i:QCOLS + D * (i + 1)]
    q_mine = jnp.concatenate([q_rows[pl.ds(pl.multiple_of(HEADS * b + MY * core, 8), MY), :] for b in range(ROWS)], axis=0)
    s_new = jnp.sum(q_mine * k_exp[...], axis=1, keepdims=True)

    tick = (lax.broadcasted_iota(jnp.int32, (16, 16, D), 0) * 2
            + lax.broadcasted_iota(jnp.int32, (16, 16, D), 1) // KV).astype(F32).astype(BF16)

    def put(which, buf):
        def body(i, _):
            rows = pl.ds(pl.multiple_of(i * 16, 16), 16)
            for b in range(ROWS):
                want = (pos_smem[b] - core * SEQ - i * 32).astype(F32).astype(BF16)
                new = kv_rows[which, 2 * KV * b:2 * KV * (b + 1), :].astype(BF16)
                buf[b, rows] = jnp.where(tick == want, new[None], buf[b, rows])
            return 0
        lax.fori_loop(0, SEQ // 32, body, 0)

    put(0, kbuf)

    x_copy.wait_recv()
    stats = part_recv[ROWS]
    peer = [part_recv[0:ROWS].reshape(ROWS * MY, D)]
    for i in range(2):
        lanes = [D // (2 * ROWS) * (2 * b + i) for b in range(ROWS)]
        peer.append(jnp.concatenate([jnp.broadcast_to(stats[:, at:at + 1], (MY, D)) for at in lanes], axis=0))
    top = jnp.maximum(jnp.maximum(part_own[1], peer[1]), s_new)
    w_own = jnp.exp2((part_own[1] - top) * EXP2_SCALE)
    w_peer = jnp.exp2((peer[1] - top) * EXP2_SCALE)
    w_new = jnp.exp2((s_new - top) * EXP2_SCALE)
    total = part_own[2] * w_own + peer[2] * w_peer + w_new
    o_rows[...] = (part_own[0] * w_own + peer[0] * w_peer + v_exp[...] * w_new) / total

    o_lhs[...] = jnp.zeros_like(o_lhs)
    for h in range(MY):
        o_lhs[0:ROWS, D * h:D * (h + 1)] = o_rows[pl.ds(h, ROWS, stride=MY), :]
    o_bf = o_lhs[...].astype(BF16)

    def p_copy(n):
        cols = pl.ds(OUT_PARTS[n][0], OUT_PARTS[n][1])
        return pltpu.make_async_remote_copy(out_send.at[:, cols], out_recv.at[:, cols], send_p, recv_p,
                                            device_id=dev(0, 1), device_id_type=MESH)

    for n, (at, width) in enumerate(OUT_PARTS):
        wo_copy(n).wait()
        out_send[:, at:at + width] = jnp.dot(o_bf, w_o[:, at:at + width], preferred_element_type=F32)[0:ROWS]
        p_copy(n).start()
    put(1, vbuf)
    whole(out_recv, send_p, recv_p).wait_recv()
    attn_out[...] = (out_send[...] + out_recv[...]).astype(BF16)

    whole(gather.at[1:CHIPS, core], send_a, recv_a.at[0]).wait_send()
    whole(gather.at[1:CHIPS, core], send_f, recv_f).wait_send()
    whole(proj_recv.at[0:len(peers)], send_b, recv_b).wait_send()
    x_copy.wait_send()
    whole(out_send, send_p, recv_p).wait_send()


def finish_kernel(attn, k_old, v_old, attn_out, k_next, v_next, sem):
    copies = [pltpu.make_async_copy(src, dst, sem.at[i])
              for i, (src, dst) in enumerate(((k_old, k_next), (v_old, v_next), (attn, attn_out)))]
    for cp in copies:
        cp.start()
    for cp in copies:
        cp.wait()


def solution(mesh):
    row_spec = P(('rep', 'dp'), None)
    cache_spec = P(('rep', 'dp'), 'sp', None, None)
    len_spec = P(('rep', 'dp'))
    y_stride = 4 if mesh.shape['dp'] >= 8 else 2

    def local_step(hidden, w_query, w_key, w_value, w_out, k_cache, v_cache, write_pos, valid_len):
        shape = k_cache.shape
        pairs = (ROWS, SEQ * KV // 16, 16, D)
        any_spec = pl.BlockSpec(memory_space=pl.ANY)
        vmem = pltpu.VMEM
        dma = pltpu.SemaphoreType.DMA
        attn, k_old, v_old = pl.pallas_call(
            functools.partial(step_kernel, y_stride),
            out_shape=[vmem(hidden.shape, BF16), vmem(pairs, BF16), vmem(pairs, BF16)],
            in_specs=[any_spec] * 8,
            out_specs=[pl.BlockSpec(memory_space=vmem)] * 3,
            scratch_shapes=[
                pltpu.SMEM((ROWS,), jnp.int32),
                vmem((CHIPS, 2, ROWS, HALF), BF16),
                vmem((2, CHIPS * ROWS, HALF), F32),
                vmem((WIDTH, COLS), BF16),
                vmem((CHIPS * ROWS, COLS), F32),
                vmem((CHIPS, ROWS, COLS), BF16),
                vmem((KV, ROWS, COLS), BF16),
                vmem((ROWS * HEADS, D), F32),
                vmem((ROWS, D, SEQ * KV), BF16),
                vmem((HALF, WIDTH), BF16),
                vmem((ROWS + 1, MY, D), F32),
                vmem((ROWS + 1, MY, D), F32),
                vmem((3, ROWS * MY, D), F32),
                vmem((ROWS * MY, D), F32),
                vmem((ROWS * MY, D), F32),
                vmem((2, ROWS * 2 * KV, D), F32),
                vmem((ROWS * MY, D), F32),
                vmem((16, HALF), F32),
                vmem((ROWS, WIDTH), F32),
                vmem((ROWS, WIDTH), F32),
                dma((3,)), dma, dma((2,)), dma((len(OUT_PARTS),)),
                dma, dma((CHIPS - 1,)), dma, dma, dma, dma, dma, dma, dma, dma,
            ],
            compiler_params=pltpu.CompilerParams(
                collective_id=0, has_side_effects=True, vmem_limit_bytes=56 * 1024 * 1024),
            cost_estimate=pl.CostEstimate(flops=10 ** 9, bytes_accessed=6 * 10 ** 7, transcendentals=10 ** 6),
        )(hidden, w_query, w_key, w_value, w_out, k_cache.reshape(pairs), v_cache.reshape(pairs), write_pos)
        return pl.pallas_call(
            finish_kernel,
            out_shape=[jax.ShapeDtypeStruct(hidden.shape, BF16)] + [jax.ShapeDtypeStruct(shape, BF16)] * 2,
            in_specs=[any_spec] * 3,
            out_specs=[any_spec] * 3,
            scratch_shapes=[dma((3,))],
            compiler_params=pltpu.CompilerParams(vmem_limit_bytes=1024 * 1024),
            cost_estimate=pl.CostEstimate(flops=10 ** 6, bytes_accessed=10 ** 7, transcendentals=0),
        )(attn, k_old.reshape(shape), v_old.reshape(shape))

    return jax.shard_map(local_step, mesh=mesh, in_specs=(row_spec, P(), P(), P(), P('sp', None), cache_spec, cache_spec, len_spec, len_spec), out_specs=(row_spec, cache_spec, cache_spec), check_vma=False)
```
